32 devices in a mesh: dp: 2 (over x), ei: 4 (over z), eo: 4 (over y, core).
Axes of the slice: x: 2, y: 2, z: 4, core: 2. Of those that a mesh axis runs over, the one named last changes fastest.
Arguments:
- x_in: bfloat16 [8192, 1024], P(('dp', 'ei', 'eo')), parts along dimension 0
- expert_idx: int32 [8192, 8], P(('dp', 'ei', 'eo')), parts along dimension 0
- gate_val: float32 [8192, 8], P(('dp', 'ei', 'eo')), parts along dimension 0
- w_gate: bfloat16 [32, 1024, 512], P(('ei', 'eo'))
- w_up: bfloat16 [32, 1024, 512], P(('ei', 'eo'))
- w_down: bfloat16 [32, 512, 1024], P(('ei', 'eo'))
- dy_in: bfloat16 [8192, 1024], P(('dp', 'ei', 'eo')), parts along dimension 0
Outputs:
- output 1: bfloat16 [8192, 1024], P(('dp', 'ei', 'eo')), parts along dimension 0
- output 2: bfloat16 [8192, 1024], P(('dp', 'ei', 'eo')), parts along dimension 0
- output 3: float32 [8192, 8], P(('dp', 'ei', 'eo')), parts along dimension 0
- output 4: float32 [64, 1024, 512], P(('dp', 'ei', 'eo')), parts along dimension 0
- output 5: float32 [64, 1024, 512], P(('dp', 'ei', 'eo')), parts along dimension 0
- output 6: float32 [64, 512, 1024], P(('dp', 'ei', 'eo')), parts along dimension 0
There are 2 independent parts. The reference program is written for one: setup_inputs(seed, part) draws one part's arguments, and reference() takes and returns one part's arrays. A program takes and returns all parts, laid end to end along the dimension named above; an argument that names none is the same for every part.
All inputs are finite; a program needn't handle non-finite values.
Results may differ from the reference program's by a relative error of at most 0.00783561.
Values are sent between devices in bfloat16 or wider.
A program may use at most 1 GiB of HBM per device.

```python
import jax
import jax.numpy as jnp
from jax import lax

TOKENS_DEV = 256
GROUP_DEVS = 16
D_MODEL = 1024
FF_EXPERT = 512
EXPERTS = 32
TOP_K = 8
SKEW_FACTOR = 4

CAPACITY = SKEW_FACTOR * ((TOKENS_DEV * TOP_K + EXPERTS - 1) // EXPERTS)
ROWS_EXPERT = GROUP_DEVS * CAPACITY
HOT_EXPERTS = EXPERTS // 8
REST_LOAD = TOKENS_DEV * TOP_K - HOT_EXPERTS * CAPACITY
REST_BASE = REST_LOAD // (EXPERTS - HOT_EXPERTS)
REST_EXTRA = REST_LOAD % (EXPERTS - HOT_EXPERTS)


def draw_routing(dev_key):
    perm_key, tok_key, col_key = jax.random.split(dev_key, 3)
    rank_ids = jnp.arange(EXPERTS, dtype=jnp.int32)
    extra_one = ((rank_ids - HOT_EXPERTS) < REST_EXTRA).astype(jnp.int32)
    load_by_rank = jnp.where(rank_ids < HOT_EXPERTS, CAPACITY, REST_BASE + extra_one).astype(jnp.int32)
    expert_perm = jax.random.permutation(perm_key, EXPERTS)
    exp_loads = jnp.zeros((EXPERTS,), jnp.int32).at[expert_perm].set(load_by_rank)
    load_ends = jnp.cumsum(exp_loads)
    positions = jnp.arange(TOKENS_DEV * TOP_K, dtype=jnp.int32)
    expert_list = jnp.searchsorted(load_ends, positions, side='right').astype(jnp.int32)
    base_idx = expert_list.reshape(TOP_K, TOKENS_DEV).T
    tok_perm = jax.random.permutation(tok_key, TOKENS_DEV)
    col_score = jax.random.randint(col_key, (TOKENS_DEV, TOP_K), 0, 1 << 20) * TOP_K + jnp.arange(TOP_K, dtype=jnp.int32)
    col_perm = jnp.argsort(col_score, axis=1)
    return jnp.take_along_axis(base_idx[tok_perm], col_perm, axis=1).astype(jnp.int32)


def setup_inputs(seed: int = 0, part: int = 0) -> dict:
    root_key = jax.random.key(seed)
    part_root, shared_root = jax.random.split(root_key)
    part_key = jax.random.fold_in(part_root, part)
    x_key, route_key, gate_key, dy_key = jax.random.split(part_key, 4)
    wg_key, wu_key, wd_key = jax.random.split(shared_root, 3)
    n_tok = GROUP_DEVS * TOKENS_DEV
    dev_keys = jax.random.split(route_key, GROUP_DEVS)
    expert_idx = jax.vmap(draw_routing)(dev_keys).reshape(n_tok, TOP_K)
    x_in = jax.random.normal(x_key, (n_tok, D_MODEL), jnp.float32).astype(jnp.bfloat16)
    gate_val = jax.random.uniform(gate_key, (n_tok, TOP_K), jnp.float32, 0.05, 0.3)
    w_gate = (jax.random.normal(wg_key, (EXPERTS, D_MODEL, FF_EXPERT), jnp.float32) * D_MODEL ** -0.5).astype(jnp.bfloat16)
    w_up = (jax.random.normal(wu_key, (EXPERTS, D_MODEL, FF_EXPERT), jnp.float32) * D_MODEL ** -0.5).astype(jnp.bfloat16)
    w_down = (jax.random.normal(wd_key, (EXPERTS, FF_EXPERT, D_MODEL), jnp.float32) * FF_EXPERT ** -0.5).astype(jnp.bfloat16)
    dy_in = jax.random.normal(dy_key, (n_tok, D_MODEL), jnp.float32).astype(jnp.bfloat16)
    return {'x_in': x_in, 'expert_idx': expert_idx, 'gate_val': gate_val, 'w_gate': w_gate, 'w_up': w_up, 'w_down': w_down, 'dy_in': dy_in}


def expert_pass(x_rows, do_rows, w_gate_e, w_up_e, w_down_e):
    pre_gate = jnp.dot(x_rows, w_gate_e, preferred_element_type=jnp.float32)
    pre_up = jnp.dot(x_rows, w_up_e, preferred_element_type=jnp.float32)
    sig_gate = jax.nn.sigmoid(pre_gate)
    silu_gate = pre_gate * sig_gate
    hidden = (silu_gate * pre_up).astype(jnp.bfloat16)
    out_rows = jnp.dot(hidden, w_down_e, preferred_element_type=jnp.float32).astype(jnp.bfloat16)
    dw_down_e = jnp.dot(hidden.T, do_rows, preferred_element_type=jnp.float32)
    d_hidden = jnp.dot(do_rows, w_down_e.T, preferred_element_type=jnp.float32)
    d_gate = (d_hidden * pre_up * sig_gate * (1.0 + pre_gate * (1.0 - sig_gate))).astype(jnp.bfloat16)
    d_up = (d_hidden * silu_gate).astype(jnp.bfloat16)
    dw_gate_e = jnp.dot(x_rows.T, d_gate, preferred_element_type=jnp.float32)
    dw_up_e = jnp.dot(x_rows.T, d_up, preferred_element_type=jnp.float32)
    dx_rows = (jnp.dot(d_gate, w_gate_e.T, preferred_element_type=jnp.float32) + jnp.dot(d_up, w_up_e.T, preferred_element_type=jnp.float32)).astype(jnp.bfloat16)
    return out_rows, dx_rows, dw_gate_e, dw_up_e, dw_down_e


def reference(x_in, expert_idx, gate_val, w_gate, w_up, w_down, dy_in):
    n_tok = GROUP_DEVS * TOKENS_DEV
    n_assign = n_tok * TOP_K
    flat_exp = expert_idx.reshape(n_assign)
    sort_order = jnp.argsort(flat_exp, stable=True).astype(jnp.int32)
    sorted_exp = flat_exp[sort_order]
    counts = jax.ops.segment_sum(jnp.ones((n_assign,), jnp.int32), flat_exp, num_segments=EXPERTS)
    starts = jnp.cumsum(counts) - counts
    within = jnp.arange(n_assign, dtype=jnp.int32) - starts[sorted_exp]
    slot_sorted = (sorted_exp * ROWS_EXPERT + within).astype(jnp.int32)
    slot_of = jnp.zeros((n_assign,), jnp.int32).at[sort_order].set(slot_sorted)
    slot_owner = jnp.full((EXPERTS * ROWS_EXPERT,), -1, jnp.int32).at[slot_sorted].set(sort_order)
    has_row = slot_owner >= 0
    safe_owner = jnp.where(has_row, slot_owner, 0)
    tok_of_slot = safe_owner // TOP_K
    slot_gate = jnp.where(has_row, gate_val.reshape(n_assign)[safe_owner], 0.0)

    def one_expert(operands):
        tok_ids, gate_rows, w_gate_e, w_up_e, w_down_e = operands
        x_rows = x_in[tok_ids]
        do_rows = (gate_rows[:, None] * dy_in[tok_ids]).astype(jnp.bfloat16)
        return expert_pass(x_rows, do_rows, w_gate_e, w_up_e, w_down_e)

    out_rows, dx_rows, dw_gate, dw_up, dw_down = lax.map(one_expert, (tok_of_slot.reshape(EXPERTS, ROWS_EXPERT), slot_gate.reshape(EXPERTS, ROWS_EXPERT), w_gate, w_up, w_down))
    out_tok = out_rows.reshape(EXPERTS * ROWS_EXPERT, D_MODEL)[slot_of].reshape(n_tok, TOP_K, D_MODEL).astype(jnp.float32)
    y_out = jnp.sum(gate_val[:, :, None] * out_tok, axis=1).astype(jnp.bfloat16)
    dgate_out = jnp.sum(dy_in.astype(jnp.float32)[:, None, :] * out_tok, axis=2)
    dx_tok = dx_rows.reshape(EXPERTS * ROWS_EXPERT, D_MODEL)[slot_of].reshape(n_tok, TOP_K, D_MODEL).astype(jnp.float32)
    dx_out = jnp.sum(dx_tok, axis=1).astype(jnp.bfloat16)
    return (y_out, dx_out, dgate_out, dw_gate, dw_up, dw_down)
```

```python
import jax
import jax.numpy as jnp
from jax import lax
from jax.sharding import PartitionSpec as P

GROUP = ('ei', 'eo')


def solution(mesh):
    group_devs = mesh.shape['ei'] * mesh.shape['eo']
    eo_size = mesh.shape['eo']
    tok_spec = P(('dp', 'ei', 'eo'), None)
    weight_spec = P(('ei', 'eo'), None, None)
    grad_spec = P(('dp', 'ei', 'eo'), None, None)

    def device_layer(x_loc, idx_loc, gate_loc, wg_loc, wu_loc, wd_loc, dy_loc):
        tok_count, top_k = idx_loc.shape
        d_model = x_loc.shape[1]
        exp_local = wg_loc.shape[0]
        experts = exp_local * group_devs
        me = lax.axis_index('ei') * eo_size + lax.axis_index('eo')
        dense_gate = jnp.sum(jnp.where(idx_loc[:, :, None] == jnp.arange(experts), gate_loc[:, :, None], 0.0), axis=1)
        gate_all = lax.all_to_all(dense_gate.reshape(tok_count, group_devs, exp_local).transpose(1, 0, 2), GROUP, 0, 0, tiled=True)
        gate_all = gate_all.reshape(group_devs * tok_count, exp_local)
        x_all = lax.all_gather(x_loc, GROUP, axis=0, tiled=True)
        dy_all = lax.all_gather(dy_loc, GROUP, axis=0, tiled=True)
        y_part = jnp.zeros((group_devs * tok_count, d_model), jnp.float32)
        dx_part = jnp.zeros((group_devs * tok_count, d_model), jnp.float32)
        saved = []
        dgates = []
        for e in range(exp_local):
            gate_e = gate_all[:, e:e + 1]
            routed = gate_e > 0.0
            x_e = jnp.where(routed, x_all, 0)
            a = jnp.dot(x_e, wg_loc[e], preferred_element_type=jnp.float32)
            b = jnp.dot(x_e, wu_loc[e], preferred_element_type=jnp.float32)
            s = jax.nn.sigmoid(a)
            h = (a * s * b).astype(jnp.bfloat16)
            o = jnp.dot(h, wd_loc[e], preferred_element_type=jnp.float32).astype(jnp.bfloat16).astype(jnp.float32)
            y_part = y_part + gate_e * o
            dgates.append(jnp.sum(dy_all.astype(jnp.float32) * o, axis=1))
            saved.append((x_e, a, b, s, h, gate_e))
        y_loc = lax.psum_scatter(y_part, GROUP, scatter_dimension=0, tiled=True).astype(jnp.bfloat16)
        grads = []
        for e in range(exp_local):
            x_e, a, b, s, h, gate_e = saved[e]
            g = jnp.where(gate_e > 0.0, (gate_e * dy_all).astype(jnp.bfloat16), 0)
            dh = lax.dot_general(g, wd_loc[e], (((1,), (1,)), ((), ())), preferred_element_type=jnp.float32)
            da = (dh * b * s * (1.0 + a * (1.0 - s))).astype(jnp.bfloat16)
            db = (dh * (a * s)).astype(jnp.bfloat16)
            dx = (lax.dot_general(da, wg_loc[e], (((1,), (1,)), ((), ())), preferred_element_type=jnp.float32)
                  + lax.dot_general(db, wu_loc[e], (((1,), (1,)), ((), ())), preferred_element_type=jnp.float32)).astype(jnp.bfloat16)
            dx_part = dx_part + dx.astype(jnp.float32)
            grads.append((x_e, da, db, h, g))
        dx_loc = lax.psum_scatter(dx_part, GROUP, scatter_dimension=0, tiled=True).astype(jnp.bfloat16)

        def tdot(p, q):
            return lax.dot_general(p, q, (((0,), (0,)), ((), ())), preferred_element_type=jnp.float32)

        dw_gate = jnp.stack([tdot(x_e, da) for x_e, da, db, h, g in grads])
        dw_up = jnp.stack([tdot(x_e, db) for x_e, da, db, h, g in grads])
        dw_down = jnp.stack([tdot(h, g) for x_e, da, db, h, g in grads])
        dg = jnp.stack(dgates, axis=1).reshape(group_devs, tok_count, exp_local)
        dg = lax.all_to_all(dg, GROUP, 0, 0, tiled=True).transpose(1, 0, 2).reshape(tok_count, experts)
        dgate_loc = jnp.sum(jnp.where(idx_loc[:, :, None] == jnp.arange(experts), dg[:, None, :], 0.0), axis=2)
        return y_loc, dx_loc, dgate_loc, dw_gate, dw_up, dw_down

    return jax.shard_map(device_layer, mesh=mesh, in_specs=(tok_spec, tok_spec, tok_spec, weight_spec, weight_spec, weight_spec, tok_spec), out_specs=(tok_spec, tok_spec, tok_spec, grad_spec, grad_spec, grad_spec), check_vma=False)
```

```python
import functools

import jax
import jax.numpy as jnp
from jax import lax
from jax.experimental import pallas as pl
from jax.experimental.pallas import tpu as pltpu
from jax.sharding import PartitionSpec as P

MESH = pl.DeviceIdType.MESH
F32 = jnp.float32
BF16 = jnp.bfloat16
SLOTS = 3


def mm(p, q, cp, cq):
    return lax.dot_general(p, q, (((cp,), (cq,)), ((), ())), preferred_element_type=F32)


def ring_kernel(n_z, x_ref, dy_ref, idx_ref, gate_ref, wg_ref, wu_ref, wd_ref,
                y_ref, dx_ref, dgate_ref, dwg_ref, dwu_ref, dwd_ref,
                xd, gt, acc, dga, part, final, dgp, dgf, wg, wu, wd, awg, awu, awd,
                load_sem, xd_send, xd_recv, gt_send, gt_recv, y_send, y_recv, dx_send, dx_recv, dg_send, dg_recv,
                credit):
    tok, top_k = idx_ref.shape
    half = tok // 2
    exp_local = wg_ref.shape[0]
    n_q = 2 * n_z
    n = 2 * n_q
    experts = exp_local * n
    z = lax.axis_index('ei')
    eo = lax.axis_index('eo')
    ycoord, core = eo // 2, eo % 2
    q = z + ycoord * (n_q - 1 - 2 * z)
    me = 2 * q + core
    first_expert = (z * 4 + eo) * exp_local

    def device_at(pos):
        pos = lax.rem(pos + 2 * n, n)
        chip, c = pos // 2, pos % 2
        col = chip // n_z
        return {'ei': chip + col * (n_q - 1 - 2 * chip), 'eo': col * 2 + c}

    right, left = device_at(me + 1), device_at(me - 1)
    to = (right, left)
    back = (left, right)

    loads = [pltpu.make_async_copy(src, dst, load_sem.at[i]) for i, (src, dst) in enumerate(
        ((x_ref, xd.at[0, 0]), (dy_ref, xd.at[0, 1]), (wg_ref, wg), (wu_ref, wu), (wd_ref, wd)))]
    for c in loads:
        c.start()

    barrier = pltpu.get_barrier_semaphore()
    for nb in (left, right):
        pl.semaphore_signal(barrier, inc=1, device_id=nb, device_id_type=MESH)

    lane = lax.broadcasted_iota(jnp.int32, (tok, 128), 1)
    dense = jnp.zeros((tok, 128), F32)
    for j in range(top_k):
        dense = dense + jnp.where(lane == idx_ref[:, j:j + 1], gate_ref[:, j:j + 1], 0.0)
    for d in range(2):
        gt[0, d] = dense[d * half:(d + 1) * half].T[:experts]
    for e in range(exp_local):
        awg[e] = jnp.zeros(awg.shape[1:], F32)
        awu[e] = jnp.zeros(awu.shape[1:], F32)
        awd[e] = jnp.zeros(awd.shape[1:], F32)

    pl.semaphore_wait(barrier, 2)
    loads[0].wait()
    loads[1].wait()

    def rows(d):
        return pl.ds(d * half, half)

    def xd_copy(s, d):
        return pltpu.make_async_remote_copy(
            src_ref=xd.at[s, :, rows(d)], dst_ref=xd.at[s + 1, :, rows(d)], send_sem=xd_send.at[s, d],
            recv_sem=xd_recv.at[s, d], device_id=to[d], device_id_type=MESH)

    def gt_copy(s, d):
        return pltpu.make_async_remote_copy(
            src_ref=gt.at[s, d], dst_ref=gt.at[s + 1, d], send_sem=gt_send.at[s, d],
            recv_sem=gt_recv.at[s, d], device_id=to[d], device_id_type=MESH)

    def acc_copy(s, d, k):
        send, recv = ((y_send, y_recv), (dx_send, dx_recv))[k]
        return pltpu.make_async_remote_copy(
            src_ref=acc.at[lax.rem(s, SLOTS), k, rows(d)], dst_ref=acc.at[lax.rem(s + 1, SLOTS), k, rows(d)],
            send_sem=send.at[s, d], recv_sem=recv.at[s, d], device_id=to[d], device_id_type=MESH)

    def dg_copy(s, d):
        return pltpu.make_async_remote_copy(
            src_ref=dga.at[lax.rem(s, SLOTS), d], dst_ref=dga.at[lax.rem(s + 1, SLOTS), d],
            send_sem=dg_send.at[s, d], recv_sem=dg_recv.at[s, d], device_id=to[d], device_id_type=MESH)

    def compute(s):
        wide = [jnp.concatenate([gt[s, d], jnp.zeros((128 - experts, half), F32)], axis=0).T for d in range(2)]
        gates = jnp.concatenate(wide, axis=0)

        def one(e, carry):
            dgs = carry
            lane_t = lax.broadcasted_iota(jnp.int32, (tok, 128), 1)
            mine = lane_t == first_expert + e
            gcol = jnp.sum(jnp.where(mine, gates, 0.0), axis=1, keepdims=True)
            routed = gcol > 0.0
            x = xd[s, 0]
            a = mm(x, wg[e], 1, 0)
            b = mm(x, wu[e], 1, 0)
            sig = jax.nn.sigmoid(a)
            silu = a * sig
            h = jnp.where(routed, silu * b, 0.0).astype(BF16)
            o = mm(h, wd[e], 1, 0).astype(BF16).astype(F32)
            dyf = xd[s, 1].astype(F32)
            part[0] = jnp.where(e == 0, 0.0, part[0]) + gcol * o
            dg = jnp.sum(dyf * o, axis=1, keepdims=True)
            dgs = dgs + jnp.where(mine, dg, 0.0)
            g = (gcol * dyf).astype(BF16)
            awd[e] = awd[e] + mm(h, g, 0, 0)
            dh = mm(g, wd[e], 1, 1)
            da = jnp.where(routed, dh * b * sig * (1.0 + a * (1.0 - sig)), 0.0).astype(BF16)
            db = jnp.where(routed, dh * silu, 0.0).astype(BF16)
            awg[e] = awg[e] + mm(x, da, 0, 0)
            awu[e] = awu[e] + mm(x, db, 0, 0)
            dxr = (mm(da, wg[e], 1, 1) + mm(db, wu[e], 1, 1)).astype(BF16).astype(F32)
            part[1] = jnp.where(e == 0, 0.0, part[1]) + dxr
            return dgs

        dgs = lax.fori_loop(0, exp_local, one, jnp.zeros((tok, 128), F32))
        for d in range(2):
            dgp[d] = dgs[d * half:(d + 1) * half].T[:experts]

    for c in loads[2:]:
        c.wait()

    def step(s, carry):
        slot = lax.rem(s, SLOTS)

        @pl.when(s >= 1)
        def _():
            for d in range(2):
                xd_copy(s - 1, d).wait_recv()
                gt_copy(s - 1, d).wait_recv()

        @pl.when(s <= n - 2)
        def _():
            for d in range(2):
                gt_copy(s, d).start()
                xd_copy(s, d).start()

        compute(s)

        @pl.when(s >= 2)
        def _():
            for d in range(2):
                for k in range(2):
                    acc_copy(s - 1, d, k).wait_send()
                dg_copy(s - 1, d).wait_send()

        @pl.when(jnp.logical_and(s >= 2, s - 1 + SLOTS <= n))
        def _():
            for d in range(2):
                pl.semaphore_signal(credit.at[d], inc=1, device_id=back[d], device_id_type=MESH)

        @pl.when(s == 0)
        def _():
            final[...] = part[...]
            dgf[...] = dgp[...]

        @pl.when(jnp.logical_and(s >= 1, s + 1 - SLOTS >= 1))
        def _():
            for d in range(2):
                pl.semaphore_wait(credit.at[d], 1)

        @pl.when(s == 1)
        def _():
            acc[slot] = part[...]
            dga[slot] = dgp[...]
            for d in range(2):
                for k in range(2):
                    acc_copy(s, d, k).start()
                dg_copy(s, d).start()

        @pl.when(s >= 2)
        def _():
            for k in range(2):
                for d in range(2):
                    acc_copy(s - 1, d, k).wait_recv()
                    acc[slot, k, rows(d)] = acc[slot, k, rows(d)] + part[k, rows(d)]
                    acc_copy(s, d, k).start()
            for d in range(2):
                dg_copy(s - 1, d).wait_recv()
                dga[slot, d] = dga[slot, d] + dgp[d]
                dg_copy(s, d).start()

        @pl.when(s >= 1)
        def _():
            for d in range(2):
                xd_copy(s - 1, d).wait_send()
                gt_copy(s - 1, d).wait_send()

        return carry

    lax.fori_loop(0, n, step, 0)

    stores = [pltpu.make_async_copy(src, dst, load_sem.at[i]) for i, (src, dst) in enumerate(
        ((awg, dwg_ref), (awu, dwu_ref), (awd, dwd_ref)))]
    for c in stores:
        c.start()
    last = n % SLOTS
    for d in range(2):
        for k in range(2):
            acc_copy(n - 1, d, k).wait_send()
        dg_copy(n - 1, d).wait_send()
    for d in range(2):
        for k in range(2):
            acc_copy(n - 1, d, k).wait_recv()
        dg_copy(n - 1, d).wait_recv()
    y_ref[...] = (acc[last, 0] + final[0]).astype(BF16)
    dx_ref[...] = (acc[last, 1] + final[1]).astype(BF16)
    cols = []
    for d in range(2):
        cols.append(jnp.concatenate([dga[last, d] + dgf[d], jnp.zeros((128 - experts, half), F32)], axis=0).T)
    dg_all = jnp.concatenate(cols, axis=0)
    for j in range(top_k):
        dgate_ref[:, j:j + 1] = jnp.sum(jnp.where(lane == idx_ref[:, j:j + 1], dg_all, 0.0), axis=1, keepdims=True)
    for c in stores:
        c.wait()


def solution(mesh):
    n_z = mesh.shape['ei']
    n = n_z * mesh.shape['eo']
    tok_spec = P(('dp', 'ei', 'eo'), None)
    weight_spec = P(('ei', 'eo'), None, None)
    grad_spec = P(('dp', 'ei', 'eo'), None, None)

    def device_layer(x_loc, idx_loc, gate_loc, wg_loc, wu_loc, wd_loc, dy_loc):
        tok, top_k = idx_loc.shape
        d_model = x_loc.shape[1]
        exp_local, _, ff = wg_loc.shape
        experts = exp_local * n
        half = tok // 2
        hbm = pl.BlockSpec(memory_space=pl.ANY)
        vm = pl.BlockSpec(memory_space=pltpu.VMEM)
        dma = pltpu.SemaphoreType.DMA
        y, dx, dgate, dwg, dwu, dwd = pl.pallas_call(
            functools.partial(ring_kernel, n_z),
            out_shape=(jax.ShapeDtypeStruct((tok, d_model), BF16), jax.ShapeDtypeStruct((tok, d_model), BF16),
                       jax.ShapeDtypeStruct((tok, top_k), F32), jax.ShapeDtypeStruct(wg_loc.shape, F32),
                       jax.ShapeDtypeStruct(wu_loc.shape, F32), jax.ShapeDtypeStruct(wd_loc.shape, F32)),
            in_specs=[hbm, hbm, vm, vm, hbm, hbm, hbm],
            out_specs=(vm, vm, vm, hbm, hbm, hbm),
            scratch_shapes=[
                pltpu.VMEM((n, 2, tok, d_model), BF16),
                pltpu.VMEM((n, 2, experts, half), F32),
                pltpu.VMEM((SLOTS, 2, tok, d_model), F32),
                pltpu.VMEM((SLOTS, 2, experts, half), F32),
                pltpu.VMEM((2, tok, d_model), F32),
                pltpu.VMEM((2, tok, d_model), F32),
                pltpu.VMEM((2, experts, half), F32),
                pltpu.VMEM((2, experts, half), F32),
                pltpu.VMEM(wg_loc.shape, BF16), pltpu.VMEM(wu_loc.shape, BF16), pltpu.VMEM(wd_loc.shape, BF16),
                pltpu.VMEM(wg_loc.shape, F32), pltpu.VMEM(wu_loc.shape, F32), pltpu.VMEM(wd_loc.shape, F32),
                dma((5,)),
                dma((n, 2)), dma((n, 2)), dma((n, 2)), dma((n, 2)), dma((n, 2)), dma((n, 2)),
                dma((n, 2)), dma((n, 2)), dma((n, 2)), dma((n, 2)),
                pltpu.SemaphoreType.REGULAR((2,)),
            ],
            compiler_params=pltpu.CompilerParams(collective_id=0, has_side_effects=True, vmem_limit_bytes=60 * 1024 * 1024),
        )(x_loc, dy_loc, idx_loc, gate_loc, wg_loc, wu_loc, wd_loc)
        return y, dx, dgate, dwg, dwu, dwd

    return jax.shard_map(device_layer, mesh=mesh, in_specs=(tok_spec, tok_spec, tok_spec, weight_spec, weight_spec, weight_spec, tok_spec), out_specs=(tok_spec, tok_spec, tok_spec, grad_spec, grad_spec, grad_spec), check_vma=False)
```

```python
import functools

import jax
import jax.numpy as jnp
from jax import lax
from jax.experimental import pallas as pl
from jax.experimental.pallas import tpu as pltpu
from jax.sharding import PartitionSpec as P

MESH = pl.DeviceIdType.MESH
F32 = jnp.float32
BF16 = jnp.bfloat16
SLOTS = 3


def mm(p, q, cp, cq):
    return lax.dot_general(p, q, (((cp,), (cq,)), ((), ())), preferred_element_type=F32)


def ring_kernel(n_z, x_ref, dy_ref, idx_ref, gate_ref, wg_ref, wu_ref, wd_ref,
                y_ref, dx_ref, dgate_ref, awg, awu, awd,
                xd, gt, acc, dga, part, dgp, pb, dgb, wg, wu, wd,
                load_sem, xd_send, xd_recv, gt_send, gt_recv, y_send, y_recv, dx_send, dx_recv, dg_send, dg_recv, pb_recv, credit):
    top_k, tok = idx_ref.shape
    half = tok // 2
    exp_local = wg_ref.shape[0]
    n_q = 2 * n_z
    n = 2 * n_q
    experts = exp_local * n
    z = lax.axis_index('ei')
    eo = lax.axis_index('eo')
    ycoord, core = eo // 2, eo % 2
    q = z + ycoord * (n_q - 1 - 2 * z)
    me = 2 * q + core
    first_expert = (z * 4 + eo) * exp_local

    def device_at(pos):
        pos = lax.rem(pos + 2 * n, n)
        chip, c = pos // 2, pos % 2
        col = chip // n_z
        return {'ei': chip + col * (n_q - 1 - 2 * chip), 'eo': col * 2 + c}

    right, left = device_at(me + 1), device_at(me - 1)
    to = (right, left)
    back = (left, right)
    partner = {'ei': z, 'eo': eo + 1 - 2 * core}
    leaves = (core == 1, core == 0)

    loads = [pltpu.make_async_copy(src, dst, load_sem.at[i]) for i, (src, dst) in enumerate(
        ((x_ref, xd.at[0, 0]), (dy_ref, xd.at[0, 1]), (wg_ref, wg), (wu_ref, wu), (wd_ref, wd)))]
    for c in loads:
        c.start()

    barrier = pltpu.get_barrier_semaphore()
    for nb in (left, right):
        pl.semaphore_signal(barrier, inc=1, device_id=nb, device_id_type=MESH)

    row = lax.broadcasted_iota(jnp.int32, (experts, tok), 0)
    dense = jnp.zeros((experts, tok), F32)
    for j in range(top_k):
        dense = dense + jnp.where(row == idx_ref[j:j + 1, :], gate_ref[j:j + 1, :], 0.0)
    for d in range(2):
        gt[0, d] = dense[:, d * half:(d + 1) * half]
    for e in range(exp_local):
        awg[e] = jnp.zeros(awg.shape[1:], F32)
        awu[e] = jnp.zeros(awu.shape[1:], F32)
        awd[e] = jnp.zeros(awd.shape[1:], F32)

    pl.semaphore_wait(barrier, 2)
    loads[0].wait()
    loads[1].wait()

    def rows(d):
        return pl.ds(d * half, half)

    def xd_copy(s, d):
        return pltpu.make_async_remote_copy(
            src_ref=xd.at[s, :, rows(d)], dst_ref=xd.at[s + 1, :, rows(d)], send_sem=xd_send.at[s, d],
            recv_sem=xd_recv.at[s, d], device_id=to[d], device_id_type=MESH)

    def gt_copy(s, d):
        return pltpu.make_async_remote_copy(
            src_ref=gt.at[s, d], dst_ref=gt.at[s + 1, d], send_sem=gt_send.at[s, d],
            recv_sem=gt_recv.at[s, d], device_id=to[d], device_id_type=MESH)

    def acc_copy(s, d, k):
        send, recv = ((y_send, y_recv), (dx_send, dx_recv))[k]
        return pltpu.make_async_remote_copy(
            src_ref=acc.at[lax.rem(s, SLOTS), k, rows(d)], dst_ref=acc.at[lax.rem(s + 1, SLOTS), k, rows(d)],
            send_sem=send.at[s, d], recv_sem=recv.at[s, d], device_id=to[d], device_id_type=MESH)

    def dg_copy(s, d):
        return pltpu.make_async_remote_copy(
            src_ref=dga.at[lax.rem(s, SLOTS), d], dst_ref=dga.at[lax.rem(s + 1, SLOTS), d],
            send_sem=dg_send.at[s, d], recv_sem=dg_recv.at[s, d], device_id=to[d], device_id_type=MESH)

    def xd_direct(d):
        return pltpu.make_async_remote_copy(
            src_ref=xd.at[0, :, rows(d)], dst_ref=xd.at[n - 1, :, rows(d)], send_sem=xd_send.at[n - 2, d],
            recv_sem=xd_recv.at[n - 2, d], device_id=partner, device_id_type=MESH)

    def gt_direct(d):
        return pltpu.make_async_remote_copy(
            src_ref=gt.at[0, d], dst_ref=gt.at[n - 1, d], send_sem=gt_send.at[n - 2, d],
            recv_sem=gt_recv.at[n - 2, d], device_id=partner, device_id_type=MESH)

    def pb_copy(d, k):
        return pltpu.make_async_remote_copy(
            src_ref=acc.at[1, k, rows(d)], dst_ref=pb.at[k], send_sem=(y_send, dx_send)[k].at[1, d],
            recv_sem=pb_recv.at[k], device_id=partner, device_id_type=MESH)

    def dgb_copy(d):
        return pltpu.make_async_remote_copy(
            src_ref=dga.at[1, d], dst_ref=dgb, send_sem=dg_send.at[1, d],
            recv_sem=pb_recv.at[2], device_id=partner, device_id_type=MESH)

    def compute(s):
        wide = [jnp.concatenate([gt[s, d], jnp.zeros((128 - experts, half), F32)], axis=0).T for d in range(2)]
        gates = jnp.concatenate(wide, axis=0)

        def one(e, carry):
            dgs = carry
            lane_t = lax.broadcasted_iota(jnp.int32, (tok, 128), 1)
            mine = lane_t == first_expert + e
            gcol = jnp.sum(jnp.where(mine, gates, 0.0), axis=1, keepdims=True)
            routed = gcol > 0.0
            x = xd[s, 0]
            a = mm(x, wg[e], 1, 0)
            b = mm(x, wu[e], 1, 0)
            sig = jax.nn.sigmoid(a)
            silu = a * sig
            h = jnp.where(routed, silu * b, 0.0).astype(BF16)
            o = mm(h, wd[e], 1, 0).astype(BF16).astype(F32)
            dyf = xd[s, 1].astype(F32)
            part[0] = jnp.where(e == 0, 0.0, part[0]) + gcol * o
            dg = jnp.sum(dyf * o, axis=1, keepdims=True)
            dgs = dgs + jnp.where(mine, dg, 0.0)
            g = (gcol * dyf).astype(BF16)
            awd[e] = awd[e] + mm(h, g, 0, 0)
            dh = mm(g, wd[e], 1, 1)
            da = jnp.where(routed, dh * b * sig * (1.0 + a * (1.0 - sig)), 0.0).astype(BF16)
            db = jnp.where(routed, dh * silu, 0.0).astype(BF16)
            awg[e] = awg[e] + mm(x, da, 0, 0)
            awu[e] = awu[e] + mm(x, db, 0, 0)
            dxr = (mm(da, wg[e], 1, 1) + mm(db, wu[e], 1, 1)).astype(BF16).astype(F32)
            part[1] = jnp.where(e == 0, 0.0, part[1]) + dxr
            return dgs

        dgs = lax.fori_loop(0, exp_local, one, jnp.zeros((tok, 128), F32))
        for d in range(2):
            dgp[d] = dgs[d * half:(d + 1) * half].T[:experts]

    for d in range(2):
        gt_copy(0, d).start()
        xd_copy(0, d).start()
    for d in range(2):
        @pl.when(leaves[d])
        def _(d=d):
            gt_direct(d).start()
            xd_direct(d).start()

    for c in loads[2:]:
        c.wait()

    def step(s, carry):
        slot = lax.rem(s, SLOTS)
        for d in range(2):
            xd_copy(s - 1, d).wait_recv()
            gt_copy(s - 1, d).wait_recv()
        for d in range(2):
            @pl.when(jnp.logical_or(s < n - 2, jnp.logical_and(s == n - 2, jnp.logical_not(leaves[d]))))
            def _(d=d):
                gt_copy(s, d).start()
                xd_copy(s, d).start()

        compute(s)

        @pl.when(s >= 2)
        def _():
            for d in range(2):
                for k in range(2):
                    acc_copy(s - 1, d, k).wait_send()
                dg_copy(s - 1, d).wait_send()

        @pl.when(jnp.logical_and(s >= 2, s - 1 + SLOTS <= n))
        def _():
            for d in range(2):
                pl.semaphore_signal(credit.at[d], inc=1, device_id=back[d], device_id_type=MESH)

        @pl.when(s >= SLOTS)
        def _():
            for d in range(2):
                pl.semaphore_wait(credit.at[d], 1)

        for d in range(2):
            fresh = jnp.logical_or(s == 1, jnp.logical_and(s == 2, jnp.logical_not(leaves[d])))

            @pl.when(fresh)
            def _(d=d):
                acc[slot, :, rows(d)] = part[:, rows(d)]
                dga[slot, d] = dgp[d]

            @pl.when(jnp.logical_and(s == 1, leaves[d]))
            def _(d=d):
                for k in range(2):
                    pb_copy(d, k).start()
                dgb_copy(d).start()

            @pl.when(jnp.logical_and(fresh, jnp.logical_not(jnp.logical_and(s == 1, leaves[d]))))
            def _(d=d):
                for k in range(2):
                    acc_copy(s, d, k).start()
                dg_copy(s, d).start()

        for k in range(2):
            for d in range(2):
                @pl.when(jnp.logical_or(s >= 3, jnp.logical_and(s == 2, leaves[d])))
                def _(d=d, k=k):
                    acc_copy(s - 1, d, k).wait_recv()
                    acc[slot, k, rows(d)] = acc[slot, k, rows(d)] + part[k, rows(d)]
                    acc_copy(s, d, k).start()
                    if k == 1:
                        dg_copy(s - 1, d).wait_recv()
                        dga[slot, d] = dga[slot, d] + dgp[d]
                        dg_copy(s, d).start()

        for d in range(2):
            xd_copy(s - 1, d).wait_send()
            gt_copy(s - 1, d).wait_send()

        return carry

    lax.fori_loop(1, n, step, 0)

    compute(0)
    last = n % SLOTS
    for d in range(2):
        for k in range(2):
            acc_copy(n - 1, d, k).wait_send()
        dg_copy(n - 1, d).wait_send()
    for k in range(2):
        pb_copy(0, k).wait_recv()
    dgb_copy(0).wait_recv()
    dgs = []
    for d in range(2):
        for k in range(2):
            acc_copy(n - 1, d, k).wait_recv()
            out = (y_ref, dx_ref)[k]
            out[rows(d)] = (acc[last, k, rows(d)] + part[k, rows(d)] + jnp.where(leaves[d], 0.0, pb[k])).astype(BF16)
        dg_copy(n - 1, d).wait_recv()
        dgs.append(dga[last, d] + dgp[d] + jnp.where(leaves[d], 0.0, dgb[...]))
    dg_all = jnp.concatenate(dgs, axis=1)
    for j in range(top_k):
        dgate_ref[j:j + 1, :] = jnp.sum(jnp.where(row == idx_ref[j:j + 1, :], dg_all, 0.0), axis=0, keepdims=True)


def solution(mesh):
    n_z = mesh.shape['ei']
    n = n_z * mesh.shape['eo']
    tok_spec = P(('dp', 'ei', 'eo'), None)
    weight_spec = P(('ei', 'eo'), None, None)
    grad_spec = P(('dp', 'ei', 'eo'), None, None)

    def device_layer(x_loc, idx_loc, gate_loc, wg_loc, wu_loc, wd_loc, dy_loc):
        tok, top_k = idx_loc.shape
        d_model = x_loc.shape[1]
        exp_local, _, ff = wg_loc.shape
        experts = exp_local * n
        half = tok // 2
        hbm = pl.BlockSpec(memory_space=pl.ANY)
        vm = pl.BlockSpec(memory_space=pltpu.VMEM)
        dma = pltpu.SemaphoreType.DMA
        out = pltpu.VMEM
        y, dx, dgate, dwg, dwu, dwd = pl.pallas_call(
            functools.partial(ring_kernel, n_z),
            out_shape=(out((tok, d_model), BF16), out((tok, d_model), BF16), out((top_k, tok), F32),
                       out(wg_loc.shape, F32), out(wu_loc.shape, F32), out(wd_loc.shape, F32)),
            in_specs=[hbm, hbm, vm, vm, hbm, hbm, hbm],
            out_specs=(vm, vm, vm, vm, vm, vm),
            scratch_shapes=[
                pltpu.VMEM((n, 2, tok, d_model), BF16),
                pltpu.VMEM((n, 2, experts, half), F32),
                pltpu.VMEM((SLOTS, 2, tok, d_model), F32),
                pltpu.VMEM((SLOTS, 2, experts, half), F32),
                pltpu.VMEM((2, tok, d_model), F32),
                pltpu.VMEM((2, experts, half), F32),
                pltpu.VMEM((2, half, d_model), F32),
                pltpu.VMEM((experts, half), F32),
                pltpu.VMEM(wg_loc.shape, BF16), pltpu.VMEM(wu_loc.shape, BF16), pltpu.VMEM(wd_loc.shape, BF16),
                dma((5,)),
                dma((n, 2)), dma((n, 2)), dma((n, 2)), dma((n, 2)), dma((n, 2)), dma((n, 2)),
                dma((n, 2)), dma((n, 2)), dma((n, 2)), dma((n, 2)), dma((3,)),
                pltpu.SemaphoreType.REGULAR((2,)),
            ],
            compiler_params=pltpu.CompilerParams(collective_id=0, has_side_effects=True, vmem_limit_bytes=48 * 2**20),
        )(x_loc, dy_loc, idx_loc.T, gate_loc.T, wg_loc, wu_loc, wd_loc)
        return y, dx, dgate.T, dwg, dwu, dwd

    return jax.shard_map(device_layer, mesh=mesh, in_specs=(tok_spec, tok_spec, tok_spec, weight_spec, weight_spec, weight_spec, tok_spec), out_specs=(tok_spec, tok_spec, tok_spec, grad_spec, grad_spec, grad_spec), check_vma=False)
```

```python
import functools

import jax
import jax.numpy as jnp
from jax import lax
from jax.experimental import pallas as pl
from jax.experimental.pallas import tpu as pltpu
from jax.sharding import PartitionSpec as P

MESH = pl.DeviceIdType.MESH
F32 = jnp.float32
BF16 = jnp.bfloat16
SLOTS = 3


def mm(p, q, cp, cq):
    return lax.dot_general(p, q, (((cp,), (cq,)), ((), ())), preferred_element_type=F32)


def ring_kernel(n_z, x_ref, dy_ref, idx_ref, gate_ref, wg_ref, wu_ref, wd_ref,
                y_ref, dx_ref, dgate_ref, awg, awu, awd,
                xd, gt, acc, part, pb, wg, wu, wd,
                load_sem, xd_send, xd_far, xd_recv, gt_send, gt_far, gt_recv, acc_send, acc_recv, pb_recv, credit):
    top_k, tok = idx_ref.shape
    half = tok // 2
    exp_local = wg_ref.shape[0]
    n_q = 2 * n_z
    n = 2 * n_q
    experts = exp_local * n
    z = lax.axis_index('ei')
    eo = lax.axis_index('eo')
    ycoord, core = eo // 2, eo % 2
    q = z + ycoord * (n_q - 1 - 2 * z)
    me = 2 * q + core
    first_expert = (z * 4 + eo) * exp_local

    def device_at(pos):
        pos = lax.rem(pos + 2 * n, n)
        chip, c = pos // 2, pos % 2
        col = chip // n_z
        return {'ei': chip + col * (n_q - 1 - 2 * chip), 'eo': col * 2 + c}

    right, left = device_at(me + 1), device_at(me - 1)
    to = (right, left)
    far = (device_at(me + 2), device_at(me - 2))
    back = (left, right)
    partner = {'ei': z, 'eo': eo + 1 - 2 * core}
    leaves = (core == 1, core == 0)

    loads = [pltpu.make_async_copy(src, dst, load_sem.at[i]) for i, (src, dst) in enumerate(
        ((x_ref, xd.at[0, 0]), (dy_ref, xd.at[0, 1]), (wg_ref, wg), (wu_ref, wu), (wd_ref, wd)))]
    for c in loads:
        c.start()

    barrier = pltpu.get_barrier_semaphore()
    for nb in (left, right) + far:
        pl.semaphore_signal(barrier, inc=1, device_id=nb, device_id_type=MESH)

    row = lax.broadcasted_iota(jnp.int32, (experts, tok), 0)
    dense = jnp.zeros((experts, tok), F32)
    for j in range(top_k):
        dense = dense + jnp.where(row == idx_ref[j:j + 1, :], gate_ref[j:j + 1, :], 0.0)
    for d in range(2):
        gt[0, d] = dense[:, d * half:(d + 1) * half]
        part[d, tok:tok + 8] = jnp.zeros((8, part.shape[2]), F32)
    for e in range(exp_local):
        awg[e] = jnp.zeros(awg.shape[1:], F32)
        awu[e] = jnp.zeros(awu.shape[1:], F32)
        awd[e] = jnp.zeros(awd.shape[1:], F32)

    pl.semaphore_wait(barrier, 4)
    loads[0].wait()
    loads[1].wait()

    def rows(d):
        return pl.ds(d * half, half)

    def xd_copy(s, d):
        return pltpu.make_async_remote_copy(
            src_ref=xd.at[s, :, rows(d)], dst_ref=xd.at[s + 1, :, rows(d)], send_sem=xd_send.at[s, d],
            recv_sem=xd_recv.at[s, d], device_id=to[d], device_id_type=MESH)

    def gt_copy(s, d):
        return pltpu.make_async_remote_copy(
            src_ref=gt.at[s, d], dst_ref=gt.at[s + 1, d], send_sem=gt_send.at[s, d],
            recv_sem=gt_recv.at[s, d], device_id=to[d], device_id_type=MESH)

    def xd_skip(s, d):
        return pltpu.make_async_remote_copy(
            src_ref=xd.at[s, :, rows(d)], dst_ref=xd.at[s + 2, :, rows(d)], send_sem=xd_far.at[s, d],
            recv_sem=xd_recv.at[s + 1, d], device_id=far[d], device_id_type=MESH)

    def gt_skip(s, d):
        return pltpu.make_async_remote_copy(
            src_ref=gt.at[s, d], dst_ref=gt.at[s + 2, d], send_sem=gt_far.at[s, d],
            recv_sem=gt_recv.at[s + 1, d], device_id=far[d], device_id_type=MESH)

    def acc_copy(s, d):
        return pltpu.make_async_remote_copy(
            src_ref=acc.at[lax.rem(s, SLOTS), d], dst_ref=acc.at[lax.rem(s + 1, SLOTS), d],
            send_sem=acc_send.at[s, d], recv_sem=acc_recv.at[s, d], device_id=to[d], device_id_type=MESH)

    def xd_direct(d):
        return pltpu.make_async_remote_copy(
            src_ref=xd.at[0, :, rows(d)], dst_ref=xd.at[n - 1, :, rows(d)], send_sem=xd_send.at[n - 2, d],
            recv_sem=xd_recv.at[n - 2, d], device_id=partner, device_id_type=MESH)

    def gt_direct(d):
        return pltpu.make_async_remote_copy(
            src_ref=gt.at[0, d], dst_ref=gt.at[n - 1, d], send_sem=gt_send.at[n - 2, d],
            recv_sem=gt_recv.at[n - 2, d], device_id=partner, device_id_type=MESH)

    def pb_copy(d):
        return pltpu.make_async_remote_copy(
            src_ref=acc.at[1, d], dst_ref=pb, send_sem=acc_send.at[1, d],
            recv_sem=pb_recv.at[0], device_id=partner, device_id_type=MESH)

    def add_part(e, at, val):
        for d in range(2):
            here = pl.ds(at, half)
            part[d, here] = jnp.where(e == 0, 0.0, part[d, here]) + val[d * half:(d + 1) * half]

    def compute(s):
        wide = [jnp.concatenate([gt[s, d], jnp.zeros((128 - experts, half), F32)], axis=0).T for d in range(2)]
        gates = jnp.concatenate(wide, axis=0)

        def one(e, carry):
            dgs = carry
            lane_t = lax.broadcasted_iota(jnp.int32, (tok, 128), 1)
            mine = lane_t == first_expert + e
            gcol = jnp.sum(jnp.where(mine, gates, 0.0), axis=1, keepdims=True)
            routed = gcol > 0.0
            x = xd[s, 0]
            a = mm(x, wg[e], 1, 0)
            b = mm(x, wu[e], 1, 0)
            sig = jax.nn.sigmoid(a)
            silu = a * sig
            h = jnp.where(routed, silu * b, 0.0).astype(BF16)
            o = mm(h, wd[e], 1, 0).astype(BF16).astype(F32)
            dyf = xd[s, 1].astype(F32)
            add_part(e, 0, gcol * o)
            dg = jnp.sum(dyf * o, axis=1, keepdims=True)
            dgs = dgs + jnp.where(mine, dg, 0.0)
            g = (gcol * dyf).astype(BF16)
            awd[e] = awd[e] + mm(h, g, 0, 0)
            dh = mm(g, wd[e], 1, 1)
            da = jnp.where(routed, dh * b * sig * (1.0 + a * (1.0 - sig)), 0.0).astype(BF16)
            db = jnp.where(routed, dh * silu, 0.0).astype(BF16)
            awg[e] = awg[e] + mm(x, da, 0, 0)
            awu[e] = awu[e] + mm(x, db, 0, 0)
            dxr = (mm(da, wg[e], 1, 1) + mm(db, wu[e], 1, 1)).astype(BF16).astype(F32)
            add_part(e, half, dxr)
            return dgs

        dgs = lax.fori_loop(0, exp_local, one, jnp.zeros((tok, 128), F32))
        for d in range(2):
            dgt = dgs[d * half:(d + 1) * half].T
            for i in range(experts // 8):
                part[d, tok:tok + 8, i * 128:(i + 1) * 128] = dgt[8 * i:8 * i + 8]

    for d in range(2):
        gt_copy(0, d).start()
        xd_copy(0, d).start()
    for d in range(2):
        @pl.when(leaves[d])
        def _(d=d):
            gt_direct(d).start()
            xd_direct(d).start()

        @pl.when(jnp.logical_not(leaves[d]))
        def _(d=d):
            gt_skip(0, d).start()
            xd_skip(0, d).start()

    for c in loads[2:]:
        c.wait()

    def step(s, carry):
        slot = lax.rem(s, SLOTS)
        for d in range(2):
            gt_copy(s - 1, d).wait_recv()
            xd_copy(s - 1, d).wait_recv()

            @pl.when(jnp.logical_and(s <= n - 2, jnp.logical_not(leaves[d])))
            def _(d=d):
                gt_copy(s, d).start()
                xd_copy(s, d).start()

            @pl.when(jnp.logical_and(s <= n - 4, jnp.logical_not(leaves[d])))
            def _(d=d):
                gt_skip(s, d).start()
                xd_skip(s, d).start()

        compute(s)

        @pl.when(s >= 2)
        def _():
            for d in range(2):
                acc_copy(s - 1, d).wait_send()

        @pl.when(jnp.logical_and(s >= 2, s - 1 + SLOTS <= n))
        def _():
            for d in range(2):
                pl.semaphore_signal(credit.at[d], inc=1, device_id=back[d], device_id_type=MESH)

        @pl.when(s >= SLOTS)
        def _():
            for d in range(2):
                pl.semaphore_wait(credit.at[d], 1)

        for d in range(2):
            fresh = jnp.logical_or(s == 1, jnp.logical_and(s == 2, jnp.logical_not(leaves[d])))

            @pl.when(fresh)
            def _(d=d):
                acc[slot, d] = part[d]

            @pl.when(jnp.logical_not(fresh))
            def _(d=d):
                acc_copy(s - 1, d).wait_recv()
                acc[slot, d] = acc[slot, d] + part[d]

            @pl.when(jnp.logical_and(s == 1, leaves[d]))
            def _(d=d):
                pb_copy(d).start()

            @pl.when(jnp.logical_not(jnp.logical_and(s == 1, leaves[d])))
            def _(d=d):
                acc_copy(s, d).start()

        return carry

    lax.fori_loop(1, n, step, 0)

    compute(0)

    def drain(s, carry):
        for d in range(2):
            @pl.when(jnp.logical_or(jnp.logical_or(s == 0, s == n - 2), jnp.logical_not(leaves[d])))
            def _(d=d):
                gt_copy(s, d).wait_send()
                xd_copy(s, d).wait_send()

            @pl.when(jnp.logical_and(s <= n - 4, jnp.logical_not(leaves[d])))
            def _(d=d):
                gt_skip(s, d).wait_send()
                xd_skip(s, d).wait_send()

        return carry

    lax.fori_loop(0, n - 1, drain, 0)
    last = n % SLOTS
    for d in range(2):
        acc_copy(n - 1, d).wait_send()
    pb_copy(0).wait_recv()
    dgs = []
    for d in range(2):
        acc_copy(n - 1, d).wait_recv()
        for k, out in enumerate((y_ref, dx_ref)):
            here = pl.ds(k * half, half)
            out[rows(d)] = (acc[last, d, here] + part[d, here] + jnp.where(leaves[d], 0.0, pb[here])).astype(BF16)
        tail = acc[last, d, tok:tok + 8] + part[d, tok:tok + 8] + jnp.where(leaves[d], 0.0, pb[tok:tok + 8])
        dgs.append(jnp.concatenate([tail[:, i * 128:(i + 1) * 128] for i in range(experts // 8)], axis=0))
    dg_all = jnp.concatenate(dgs, axis=1)
    for j in range(top_k):
        dgate_ref[j:j + 1, :] = jnp.sum(jnp.where(row == idx_ref[j:j + 1, :], dg_all, 0.0), axis=0, keepdims=True)


def store_kernel(*refs):
    count = len(refs) // 2
    sems = refs[-1]
    copies = [pltpu.make_async_copy(refs[i], refs[count + i], sems.at[i]) for i in range(count)]
    for c in copies:
        c.start()
    for c in copies:
        c.wait()


def solution(mesh):
    n_z = mesh.shape['ei']
    n = n_z * mesh.shape['eo']
    tok_spec = P(('dp', 'ei', 'eo'), None)
    weight_spec = P(('ei', 'eo'), None, None)
    grad_spec = P(('dp', 'ei', 'eo'), None, None)

    def device_layer(x_loc, idx_loc, gate_loc, wg_loc, wu_loc, wd_loc, dy_loc):
        tok, top_k = idx_loc.shape
        d_model = x_loc.shape[1]
        exp_local, _, ff = wg_loc.shape
        experts = exp_local * n
        half = tok // 2
        hbm = pl.BlockSpec(memory_space=pl.ANY)
        vm = pl.BlockSpec(memory_space=pltpu.VMEM)
        dma = pltpu.SemaphoreType.DMA
        out = pltpu.VMEM
        results = pl.pallas_call(
            functools.partial(ring_kernel, n_z),
            out_shape=(out((tok, d_model), BF16), out((tok, d_model), BF16), out((top_k, tok), F32),
                       out(wg_loc.shape, F32), out(wu_loc.shape, F32), out(wd_loc.shape, F32)),
            in_specs=[hbm, hbm, vm, vm, hbm, hbm, hbm],
            out_specs=(vm, vm, vm, vm, vm, vm),
            scratch_shapes=[
                pltpu.VMEM((n, 2, tok, d_model), BF16),
                pltpu.VMEM((n, 2, experts, half), F32),
                pltpu.VMEM((SLOTS, 2, tok + 8, d_model), F32),
                pltpu.VMEM((2, tok + 8, d_model), F32),
                pltpu.VMEM((tok + 8, d_model), F32),
                pltpu.VMEM(wg_loc.shape, BF16), pltpu.VMEM(wu_loc.shape, BF16), pltpu.VMEM(wd_loc.shape, BF16),
                dma((5,)),
                dma((n, 2)), dma((n, 2)), dma((n, 2)), dma((n, 2)), dma((n, 2)), dma((n, 2)), dma((n, 2)), dma((n, 2)), dma((1,)),
                pltpu.SemaphoreType.REGULAR((2,)),
            ],
            compiler_params=pltpu.CompilerParams(collective_id=0, has_side_effects=True, vmem_limit_bytes=48 * 2**20),
        )(x_loc, dy_loc, idx_loc.T, gate_loc.T, wg_loc, wu_loc, wd_loc)
        y, dx, dgate, dwg, dwu, dwd = pl.pallas_call(
            store_kernel,
            out_shape=tuple(jax.ShapeDtypeStruct(r.shape, r.dtype) for r in results),
            in_specs=[vm] * len(results),
            out_specs=(hbm,) * len(results),
            scratch_shapes=[dma((len(results),))],
            compiler_params=pltpu.CompilerParams(vmem_limit_bytes=2**20),
        )(*[pltpu.with_memory_space_constraint(r, pltpu.VMEM) for r in results])
        return y, dx, dgate.T, dwg, dwu, dwd

    return jax.shard_map(device_layer, mesh=mesh, in_specs=(tok_spec, tok_spec, tok_spec, weight_spec, weight_spec, weight_spec, tok_spec), out_specs=(tok_spec, tok_spec, tok_spec, grad_spec, grad_spec, grad_spec), check_vma=False)
```

```python
import functools

import jax
import jax.numpy as jnp
from jax import lax
from jax.experimental import pallas as pl
from jax.experimental.pallas import tpu as pltpu
from jax.sharding import PartitionSpec as P

MESH = pl.DeviceIdType.MESH
F32 = jnp.float32
BF16 = jnp.bfloat16
SLOTS = 4


def mm(p, q, cp, cq):
    return lax.dot_general(p, q, (((cp,), (cq,)), ((), ())), preferred_element_type=F32)


def ring_kernel(n_z, x_ref, dy_ref, idx_ref, gate_ref, wg_ref, wu_ref, wd_ref,
                y_ref, dx_ref, dgate_ref, awg, awu, awd,
                xd, gt, acc, part, pb, wg, wu, wd,
                load_sem, xd_send, xd_far, xd_recv, gt_send, gt_far, gt_recv, acc_send, acc_recv, pb_recv, credit):
    top_k, tok = idx_ref.shape
    half = tok // 2
    exp_local = wg_ref.shape[0]
    n_q = 2 * n_z
    n = 2 * n_q
    experts = exp_local * n
    z = lax.axis_index('ei')
    eo = lax.axis_index('eo')
    ycoord, core = eo // 2, eo % 2
    q = z + ycoord * (n_q - 1 - 2 * z)
    me = 2 * q + core
    first_expert = (z * 4 + eo) * exp_local

    def device_at(pos):
        pos = lax.rem(pos + 2 * n, n)
        chip, c = pos // 2, pos % 2
        col = chip // n_z
        return {'ei': chip + col * (n_q - 1 - 2 * chip), 'eo': col * 2 + c}

    right, left = device_at(me + 1), device_at(me - 1)
    to = (right, left)
    far = (device_at(me + 2), device_at(me - 2))
    back = (left, right)
    partner = {'ei': z, 'eo': eo + 1 - 2 * core}
    leaves = (core == 1, core == 0)

    loads = [pltpu.make_async_copy(src, dst, load_sem.at[i]) for i, (src, dst) in enumerate(
        ((x_ref, xd.at[0, 0]), (dy_ref, xd.at[0, 1]), (wg_ref, wg), (wu_ref, wu), (wd_ref, wd)))]
    for c in loads:
        c.start()

    barrier = pltpu.get_barrier_semaphore()
    for nb in (left, right) + far:
        pl.semaphore_signal(barrier, inc=1, device_id=nb, device_id_type=MESH)

    row = lax.broadcasted_iota(jnp.int32, (experts, tok), 0)
    dense = jnp.zeros((experts, tok), F32)
    for j in range(top_k):
        dense = dense + jnp.where(row == idx_ref[j:j + 1, :], gate_ref[j:j + 1, :], 0.0)
    for d in range(2):
        gt[0, d] = dense[:, d * half:(d + 1) * half]
        part[d, tok:tok + 8] = jnp.zeros((8, part.shape[2]), F32)
    for e in range(exp_local):
        awg[e] = jnp.zeros(awg.shape[1:], F32)
        awu[e] = jnp.zeros(awu.shape[1:], F32)
        awd[e] = jnp.zeros(awd.shape[1:], F32)

    pl.semaphore_wait(barrier, 4)
    loads[0].wait()
    loads[1].wait()

    def rows(d):
        return pl.ds(d * half, half)

    def xd_copy(s, d):
        return pltpu.make_async_remote_copy(
            src_ref=xd.at[s, :, rows(d)], dst_ref=xd.at[s + 1, :, rows(d)], send_sem=xd_send.at[s, d],
            recv_sem=xd_recv.at[s, d], device_id=to[d], device_id_type=MESH)

    def gt_copy(s, d):
        return pltpu.make_async_remote_copy(
            src_ref=gt.at[s, d], dst_ref=gt.at[s + 1, d], send_sem=gt_send.at[s, d],
            recv_sem=gt_recv.at[s, d], device_id=to[d], device_id_type=MESH)

    def xd_skip(s, d):
        return pltpu.make_async_remote_copy(
            src_ref=xd.at[s, :, rows(d)], dst_ref=xd.at[s + 2, :, rows(d)], send_sem=xd_far.at[s, d],
            recv_sem=xd_recv.at[s + 1, d], device_id=far[d], device_id_type=MESH)

    def gt_skip(s, d):
        return pltpu.make_async_remote_copy(
            src_ref=gt.at[s, d], dst_ref=gt.at[s + 2, d], send_sem=gt_far.at[s, d],
            recv_sem=gt_recv.at[s + 1, d], device_id=far[d], device_id_type=MESH)

    def acc_copy(s, d):
        return pltpu.make_async_remote_copy(
            src_ref=acc.at[lax.rem(s, SLOTS), d], dst_ref=acc.at[lax.rem(s + 1, SLOTS), d],
            send_sem=acc_send.at[s, d], recv_sem=acc_recv.at[s, d], device_id=to[d], device_id_type=MESH)

    def xd_direct(d):
        return pltpu.make_async_remote_copy(
            src_ref=xd.at[0, :, rows(d)], dst_ref=xd.at[n - 1, :, rows(d)], send_sem=xd_send.at[n - 2, d],
            recv_sem=xd_recv.at[n - 2, d], device_id=partner, device_id_type=MESH)

    def gt_direct(d):
        return pltpu.make_async_remote_copy(
            src_ref=gt.at[0, d], dst_ref=gt.at[n - 1, d], send_sem=gt_send.at[n - 2, d],
            recv_sem=gt_recv.at[n - 2, d], device_id=partner, device_id_type=MESH)

    def pb_copy(d):
        return pltpu.make_async_remote_copy(
            src_ref=acc.at[1, d], dst_ref=pb, send_sem=acc_send.at[1, d],
            recv_sem=pb_recv.at[0], device_id=partner, device_id_type=MESH)

    def add_part(e, at, val):
        for d in range(2):
            here = pl.ds(at, half)
            part[d, here] = jnp.where(e == 0, 0.0, part[d, here]) + val[d * half:(d + 1) * half]

    def compute(s):
        wide = [jnp.concatenate([gt[s, d], jnp.zeros((128 - experts, half), F32)], axis=0).T for d in range(2)]
        gates = jnp.concatenate(wide, axis=0)

        def one(e, carry):
            dgs = carry
            lane_t = lax.broadcasted_iota(jnp.int32, (tok, 128), 1)
            mine = lane_t == first_expert + e
            gcol = jnp.sum(jnp.where(mine, gates, 0.0), axis=1, keepdims=True)
            routed = gcol > 0.0
            x = xd[s, 0]
            a = mm(x, wg[e], 1, 0)
            b = mm(x, wu[e], 1, 0)
            sig = jax.nn.sigmoid(a)
            silu = a * sig
            h = jnp.where(routed, silu * b, 0.0).astype(BF16)
            o = mm(h, wd[e], 1, 0).astype(BF16).astype(F32)
            dyf = xd[s, 1].astype(F32)
            add_part(e, 0, gcol * o)
            dg = jnp.sum(dyf * o, axis=1, keepdims=True)
            dgs = dgs + jnp.where(mine, dg, 0.0)
            g = (gcol * dyf).astype(BF16)
            awd[e] = awd[e] + mm(h, g, 0, 0)
            dh = mm(g, wd[e], 1, 1)
            da = jnp.where(routed, dh * b * sig * (1.0 + a * (1.0 - sig)), 0.0).astype(BF16)
            db = jnp.where(routed, dh * silu, 0.0).astype(BF16)
            awg[e] = awg[e] + mm(x, da, 0, 0)
            awu[e] = awu[e] + mm(x, db, 0, 0)
            dxr = (mm(da, wg[e], 1, 1) + mm(db, wu[e], 1, 1)).astype(BF16).astype(F32)
            add_part(e, half, dxr)
            return dgs

        dgs = lax.fori_loop(0, exp_local, one, jnp.zeros((tok, 128), F32))
        for d in range(2):
            dgt = dgs[d * half:(d + 1) * half].T
            for i in range(experts // 8):
                part[d, tok:tok + 8, i * 128:(i + 1) * 128] = dgt[8 * i:8 * i + 8]

    for d in range(2):
        gt_copy(0, d).start()
        xd_copy(0, d).start()
    for d in range(2):
        @pl.when(leaves[d])
        def _(d=d):
            gt_direct(d).start()
            xd_direct(d).start()

        @pl.when(jnp.logical_not(leaves[d]))
        def _(d=d):
            gt_skip(0, d).start()
            xd_skip(0, d).start()

    for c in loads[2:]:
        c.wait()

    def step(s, carry):
        slot = lax.rem(s, SLOTS)
        for d in range(2):
            gt_copy(s - 1, d).wait_recv()
            xd_copy(s - 1, d).wait_recv()

            @pl.when(jnp.logical_and(s <= n - 2, jnp.logical_not(leaves[d])))
            def _(d=d):
                gt_copy(s, d).start()
                xd_copy(s, d).start()

            @pl.when(jnp.logical_and(s <= n - 4, jnp.logical_not(leaves[d])))
            def _(d=d):
                gt_skip(s, d).start()
                xd_skip(s, d).start()

        compute(s)

        def pass_on(d):
            fresh = jnp.logical_or(s == 1, jnp.logical_and(s == 2, jnp.logical_not(leaves[d])))

            @pl.when(s >= SLOTS)
            def _():
                pl.semaphore_wait(credit.at[d], 1)

            @pl.when(fresh)
            def _():
                acc[slot, d] = part[d]

            @pl.when(jnp.logical_not(fresh))
            def _():
                acc_copy(s - 1, d).wait_recv()
                acc[slot, d] = acc[slot, d] + part[d]

            @pl.when(jnp.logical_and(s == 1, leaves[d]))
            def _():
                pb_copy(d).start()

            @pl.when(jnp.logical_not(jnp.logical_and(s == 1, leaves[d])))
            def _():
                acc_copy(s, d).start()

        for d, first in ((0, True), (1, True), (0, False), (1, False)):
            @pl.when(leaves[d] if first else jnp.logical_not(leaves[d]))
            def _(d=d):
                pass_on(d)

        for d in range(2):
            @pl.when(s >= 2)
            def _(d=d):
                acc_copy(s - 1, d).wait_send()

            @pl.when(jnp.logical_and(s >= 2, s - 1 + SLOTS <= n))
            def _(d=d):
                pl.semaphore_signal(credit.at[d], inc=1, device_id=back[d], device_id_type=MESH)

        return carry

    lax.fori_loop(1, n, step, 0)

    compute(0)

    def drain(s, carry):
        for d in range(2):
            @pl.when(jnp.logical_or(jnp.logical_or(s == 0, s == n - 2), jnp.logical_not(leaves[d])))
            def _(d=d):
                gt_copy(s, d).wait_send()
                xd_copy(s, d).wait_send()

            @pl.when(jnp.logical_and(s <= n - 4, jnp.logical_not(leaves[d])))
            def _(d=d):
                gt_skip(s, d).wait_send()
                xd_skip(s, d).wait_send()

        return carry

    lax.fori_loop(0, n - 1, drain, 0)
    last = n % SLOTS
    for d in range(2):
        acc_copy(n - 1, d).wait_send()
    pb_copy(0).wait_recv()
    dgs = []
    for d in range(2):
        acc_copy(n - 1, d).wait_recv()
        for k, out in enumerate((y_ref, dx_ref)):
            here = pl.ds(k * half, half)
            out[rows(d)] = (acc[last, d, here] + part[d, here] + jnp.where(leaves[d], 0.0, pb[here])).astype(BF16)
        tail = acc[last, d, tok:tok + 8] + part[d, tok:tok + 8] + jnp.where(leaves[d], 0.0, pb[tok:tok + 8])
        dgs.append(jnp.concatenate([tail[:, i * 128:(i + 1) * 128] for i in range(experts // 8)], axis=0))
    dg_all = jnp.concatenate(dgs, axis=1)
    for j in range(top_k):
        dgate_ref[j:j + 1, :] = jnp.sum(jnp.where(row == idx_ref[j:j + 1, :], dg_all, 0.0), axis=0, keepdims=True)


def store_kernel(*refs):
    count = len(refs) // 2
    sems = refs[-1]
    copies = [pltpu.make_async_copy(refs[i], refs[count + i], sems.at[i]) for i in range(count)]
    for c in copies:
        c.start()
    for c in copies:
        c.wait()


def solution(mesh):
    n_z = mesh.shape['ei']
    n = n_z * mesh.shape['eo']
    tok_spec = P(('dp', 'ei', 'eo'), None)
    weight_spec = P(('ei', 'eo'), None, None)
    grad_spec = P(('dp', 'ei', 'eo'), None, None)

    def device_layer(x_loc, idx_loc, gate_loc, wg_loc, wu_loc, wd_loc, dy_loc):
        tok, top_k = idx_loc.shape
        d_model = x_loc.shape[1]
        exp_local, _, ff = wg_loc.shape
        experts = exp_local * n
        half = tok // 2
        hbm = pl.BlockSpec(memory_space=pl.ANY)
        vm = pl.BlockSpec(memory_space=pltpu.VMEM)
        dma = pltpu.SemaphoreType.DMA
        out = pltpu.VMEM
        results = pl.pallas_call(
            functools.partial(ring_kernel, n_z),
            out_shape=(out((tok, d_model), BF16), out((tok, d_model), BF16), out((top_k, tok), F32),
                       out(wg_loc.shape, F32), out(wu_loc.shape, F32), out(wd_loc.shape, F32)),
            in_specs=[hbm, hbm, vm, vm, hbm, hbm, hbm],
            out_specs=(vm, vm, vm, vm, vm, vm),
            scratch_shapes=[
                pltpu.VMEM((n, 2, tok, d_model), BF16),
                pltpu.VMEM((n, 2, experts, half), F32),
                pltpu.VMEM((SLOTS, 2, tok + 8, d_model), F32),
                pltpu.VMEM((2, tok + 8, d_model), F32),
                pltpu.VMEM((tok + 8, d_model), F32),
                pltpu.VMEM(wg_loc.shape, BF16), pltpu.VMEM(wu_loc.shape, BF16), pltpu.VMEM(wd_loc.shape, BF16),
                dma((5,)),
                dma((n, 2)), dma((n, 2)), dma((n, 2)), dma((n, 2)), dma((n, 2)), dma((n, 2)), dma((n, 2)), dma((n, 2)), dma((1,)),
                pltpu.SemaphoreType.REGULAR((2,)),
            ],
            compiler_params=pltpu.CompilerParams(collective_id=0, has_side_effects=True, vmem_limit_bytes=48 * 2**20),
        )(x_loc, dy_loc, idx_loc.T, gate_loc.T, wg_loc, wu_loc, wd_loc)
        y, dx, dgate, dwg, dwu, dwd = pl.pallas_call(
            store_kernel,
            out_shape=tuple(jax.ShapeDtypeStruct(r.shape, r.dtype) for r in results),
            in_specs=[vm] * len(results),
            out_specs=(hbm,) * len(results),
            scratch_shapes=[dma((len(results),))],
            compiler_params=pltpu.CompilerParams(vmem_limit_bytes=2**20),
        )(*[pltpu.with_memory_space_constraint(r, pltpu.VMEM) for r in results])
        return y, dx, dgate.T, dwg, dwu, dwd

    return jax.shard_map(device_layer, mesh=mesh, in_specs=(tok_spec, tok_spec, tok_spec, weight_spec, weight_spec, weight_spec, tok_spec), out_specs=(tok_spec, tok_spec, tok_spec, grad_spec, grad_spec, grad_spec), check_vma=False)
```

```python
import functools

import jax
import jax.numpy as jnp
from jax import lax
from jax.experimental import pallas as pl
from jax.experimental.pallas import tpu as pltpu
from jax.sharding import PartitionSpec as P

MESH = pl.DeviceIdType.MESH
F32 = jnp.float32
BF16 = jnp.bfloat16
SLOTS = 4


def mm(p, q, cp, cq):
    return lax.dot_general(p, q, (((cp,), (cq,)), ((), ())), preferred_element_type=F32)


def ring_kernel(n_z, x_ref, dy_ref, idx_ref, gate_ref, wg_ref, wu_ref, wd_ref,
                y_ref, dx_ref, dgate_ref, awg, awu, awd,
                xd, gt, acc, dga, part, dgp, pb, dgb, wg, wu, wd,
                load_sem, xd_send, xd_far, xd_recv, gt_send, gt_far, gt_recv, acc_send, acc_recv, dg_send, dg_recv, pb_recv,
                credit):
    top_k, tok = idx_ref.shape
    half = tok // 2
    exp_local = wg_ref.shape[0]
    n_q = 2 * n_z
    n = 2 * n_q
    z = lax.axis_index('ei')
    eo = lax.axis_index('eo')
    ycoord, core = eo // 2, eo % 2
    q = z + ycoord * (n_q - 1 - 2 * z)
    me = 2 * q + core
    first_expert = (z * 4 + eo) * exp_local

    def device_at(pos):
        pos = lax.rem(pos + 2 * n, n)
        chip, c = pos // 2, pos % 2
        col = chip // n_z
        return {'ei': chip + col * (n_q - 1 - 2 * chip), 'eo': col * 2 + c}

    right, left = device_at(me + 1), device_at(me - 1)
    to = (right, left)
    far = (device_at(me + 2), device_at(me - 2))
    back = (left, right)
    partner = {'ei': z, 'eo': eo + 1 - 2 * core}
    leaves = (core == 1, core == 0)

    loads = [pltpu.make_async_copy(src, dst, load_sem.at[i]) for i, (src, dst) in enumerate(
        ((x_ref, xd.at[0, 0]), (dy_ref, xd.at[0, 1]), (wg_ref, wg), (wu_ref, wu), (wd_ref, wd)))]
    for c in loads:
        c.start()

    barrier = pltpu.get_barrier_semaphore()
    for nb in (left, right) + far:
        pl.semaphore_signal(barrier, inc=1, device_id=nb, device_id_type=MESH)

    for d in range(2):
        gt[0, d, :top_k] = idx_ref[:, d * half:(d + 1) * half].astype(F32)
        gt[0, d, top_k:] = gate_ref[:, d * half:(d + 1) * half]
    for e in range(exp_local):
        awg[e] = jnp.zeros(awg.shape[1:], F32)
        awu[e] = jnp.zeros(awu.shape[1:], F32)
        awd[e] = jnp.zeros(awd.shape[1:], F32)

    pl.semaphore_wait(barrier, 4)
    loads[0].wait()
    loads[1].wait()

    def rows(d):
        return pl.ds(d * half, half)

    def xd_copy(s, d):
        return pltpu.make_async_remote_copy(
            src_ref=xd.at[s, :, rows(d)], dst_ref=xd.at[s + 1, :, rows(d)], send_sem=xd_send.at[s, d],
            recv_sem=xd_recv.at[s, d], device_id=to[d], device_id_type=MESH)

    def gt_copy(s, d):
        return pltpu.make_async_remote_copy(
            src_ref=gt.at[s, d], dst_ref=gt.at[s + 1, d], send_sem=gt_send.at[s, d],
            recv_sem=gt_recv.at[s, d], device_id=to[d], device_id_type=MESH)

    def xd_skip(s, d):
        return pltpu.make_async_remote_copy(
            src_ref=xd.at[s, :, rows(d)], dst_ref=xd.at[s + 2, :, rows(d)], send_sem=xd_far.at[s, d],
            recv_sem=xd_recv.at[s + 1, d], device_id=far[d], device_id_type=MESH)

    def gt_skip(s, d):
        return pltpu.make_async_remote_copy(
            src_ref=gt.at[s, d], dst_ref=gt.at[s + 2, d], send_sem=gt_far.at[s, d],
            recv_sem=gt_recv.at[s + 1, d], device_id=far[d], device_id_type=MESH)

    def acc_copy(s, d):
        return pltpu.make_async_remote_copy(
            src_ref=acc.at[lax.rem(s, SLOTS), d], dst_ref=acc.at[lax.rem(s + 1, SLOTS), d],
            send_sem=acc_send.at[s, d], recv_sem=acc_recv.at[s, d], device_id=to[d], device_id_type=MESH)

    def dg_copy(s, d):
        return pltpu.make_async_remote_copy(
            src_ref=dga.at[lax.rem(s, SLOTS), d], dst_ref=dga.at[lax.rem(s + 1, SLOTS), d],
            send_sem=dg_send.at[s, d], recv_sem=dg_recv.at[s, d], device_id=to[d], device_id_type=MESH)

    def xd_direct(d):
        return pltpu.make_async_remote_copy(
            src_ref=xd.at[0, :, rows(d)], dst_ref=xd.at[n - 1, :, rows(d)], send_sem=xd_send.at[n - 2, d],
            recv_sem=xd_recv.at[n - 2, d], device_id=partner, device_id_type=MESH)

    def gt_direct(d):
        return pltpu.make_async_remote_copy(
            src_ref=gt.at[0, d], dst_ref=gt.at[n - 1, d], send_sem=gt_send.at[n - 2, d],
            recv_sem=gt_recv.at[n - 2, d], device_id=partner, device_id_type=MESH)

    def pb_copy(d):
        return pltpu.make_async_remote_copy(
            src_ref=acc.at[1, d], dst_ref=pb, send_sem=acc_send.at[1, d],
            recv_sem=pb_recv.at[0], device_id=partner, device_id_type=MESH)

    def dgb_copy(d):
        return pltpu.make_async_remote_copy(
            src_ref=dga.at[1, d], dst_ref=dgb, send_sem=dg_send.at[1, d],
            recv_sem=pb_recv.at[1], device_id=partner, device_id_type=MESH)

    def add_part(e, at, val):
        for d in range(2):
            here = pl.ds(at, half)
            part[d, here] = jnp.where(e == 0, 0.0, part[d, here]) + val[d * half:(d + 1) * half]

    def compute(s):
        def columns(first, fill):
            pad = jnp.full((128 - top_k, half), fill, F32)
            return jnp.concatenate(
                [jnp.concatenate([gt[s, d, first:first + top_k], pad], axis=0).T for d in range(2)], axis=0)

        ids, gates = columns(0, -1.0), columns(top_k, 0.0)

        def one(e, carry):
            dgs = carry
            mine = ids == (first_expert + e).astype(F32)
            gcol = jnp.sum(jnp.where(mine, gates, 0.0), axis=1, keepdims=True)
            routed = gcol > 0.0
            x = xd[s, 0]
            a = mm(x, wg[e], 1, 0)
            b = mm(x, wu[e], 1, 0)
            sig = jax.nn.sigmoid(a)
            silu = a * sig
            h = jnp.where(routed, silu * b, 0.0).astype(BF16)
            o = mm(h, wd[e], 1, 0).astype(BF16).astype(F32)
            dyf = xd[s, 1].astype(F32)
            add_part(e, 0, gcol * o)
            dg = jnp.sum(dyf * o, axis=1, keepdims=True)
            dgs = dgs + jnp.where(mine, dg, 0.0)
            g = (gcol * dyf).astype(BF16)
            awd[e] = awd[e] + mm(h, g, 0, 0)
            dh = mm(g, wd[e], 1, 1)
            da = jnp.where(routed, dh * b * sig * (1.0 + a * (1.0 - sig)), 0.0).astype(BF16)
            db = jnp.where(routed, dh * silu, 0.0).astype(BF16)
            awg[e] = awg[e] + mm(x, da, 0, 0)
            awu[e] = awu[e] + mm(x, db, 0, 0)
            dxr = (mm(da, wg[e], 1, 1) + mm(db, wu[e], 1, 1)).astype(BF16).astype(F32)
            add_part(e, half, dxr)
            return dgs

        dgs = lax.fori_loop(0, exp_local, one, jnp.zeros((tok, 128), F32))
        for d in range(2):
            dgp[d] = dgs[d * half:(d + 1) * half].T[:top_k]

    for d in range(2):
        gt_copy(0, d).start()
        xd_copy(0, d).start()
    for d in range(2):
        @pl.when(leaves[d])
        def _(d=d):
            gt_direct(d).start()
            xd_direct(d).start()

    for c in loads[2:]:
        c.wait()

    def step(s, carry):
        slot = lax.rem(s, SLOTS)
        for d in range(2):
            gt_copy(s - 1, d).wait_recv()
            xd_copy(s - 1, d).wait_recv()

            @pl.when(jnp.logical_and(s <= n - 2, jnp.logical_not(leaves[d])))
            def _(d=d):
                gt_copy(s, d).start()
                xd_copy(s, d).start()

            @pl.when(jnp.logical_and(s == 1, jnp.logical_not(leaves[d])))
            def _(d=d):
                gt_skip(0, d).start()
                xd_skip(0, d).start()

            @pl.when(jnp.logical_and(s <= n - 4, jnp.logical_not(leaves[d])))
            def _(d=d):
                gt_skip(s, d).start()
                xd_skip(s, d).start()

        compute(s)

        def pass_on(d):
            fresh = jnp.logical_or(s == 1, jnp.logical_and(s == 2, jnp.logical_not(leaves[d])))

            @pl.when(s >= SLOTS)
            def _():
                pl.semaphore_wait(credit.at[d], 1)

            @pl.when(fresh)
            def _():
                acc[slot, d] = part[d]
                dga[slot, d] = dgp[d]

            @pl.when(jnp.logical_not(fresh))
            def _():
                acc_copy(s - 1, d).wait_recv()
                acc[slot, d] = acc[slot, d] + part[d]
                dg_copy(s - 1, d).wait_recv()
                dga[slot, d] = dga[slot, d] + dgp[d]

            @pl.when(jnp.logical_and(s == 1, leaves[d]))
            def _():
                pb_copy(d).start()
                dgb_copy(d).start()

            @pl.when(jnp.logical_not(jnp.logical_and(s == 1, leaves[d])))
            def _():
                acc_copy(s, d).start()
                dg_copy(s, d).start()

        for d, first in ((0, True), (1, True), (0, False), (1, False)):
            @pl.when(leaves[d] if first else jnp.logical_not(leaves[d]))
            def _(d=d):
                pass_on(d)

        for d in range(2):
            @pl.when(s >= 2)
            def _(d=d):
                acc_copy(s - 1, d).wait_send()
                dg_copy(s - 1, d).wait_send()

            @pl.when(jnp.logical_and(s >= 2, s - 1 + SLOTS <= n))
            def _(d=d):
                pl.semaphore_signal(credit.at[d], inc=1, device_id=back[d], device_id_type=MESH)

        return carry

    lax.fori_loop(1, n, step, 0)

    compute(0)

    def drain(s, carry):
        for d in range(2):
            @pl.when(jnp.logical_or(jnp.logical_or(s == 0, s == n - 2), jnp.logical_not(leaves[d])))
            def _(d=d):
                gt_copy(s, d).wait_send()
                xd_copy(s, d).wait_send()

            @pl.when(jnp.logical_and(s <= n - 4, jnp.logical_not(leaves[d])))
            def _(d=d):
                gt_skip(s, d).wait_send()
                xd_skip(s, d).wait_send()

        return carry

    lax.fori_loop(0, n - 1, drain, 0)
    last = n % SLOTS
    for d in range(2):
        acc_copy(n - 1, d).wait_send()
        dg_copy(n - 1, d).wait_send()
    pb_copy(0).wait_recv()
    dgb_copy(0).wait_recv()
    for d in range(2):
        dg_copy(n - 1, d).wait_recv()
        dgate_ref[:, d * half:(d + 1) * half] = dga[last, d] + dgp[d] + jnp.where(leaves[d], 0.0, dgb[...])
        acc_copy(n - 1, d).wait_recv()
        for k, out in enumerate((y_ref, dx_ref)):
            here = pl.ds(k * half, half)
            out[rows(d)] = (acc[last, d, here] + part[d, here] + jnp.where(leaves[d], 0.0, pb[here])).astype(BF16)


def store_kernel(*refs):
    count = len(refs) // 2
    sems = refs[-1]
    copies = [pltpu.make_async_copy(refs[i], refs[count + i], sems.at[i]) for i in range(count)]
    for c in copies:
        c.start()
    for c in copies:
        c.wait()


def solution(mesh):
    n_z = mesh.shape['ei']
    n = n_z * mesh.shape['eo']
    tok_spec = P(('dp', 'ei', 'eo'), None)
    weight_spec = P(('ei', 'eo'), None, None)
    grad_spec = P(('dp', 'ei', 'eo'), None, None)

    def device_layer(x_loc, idx_loc, gate_loc, wg_loc, wu_loc, wd_loc, dy_loc):
        tok, top_k = idx_loc.shape
        d_model = x_loc.shape[1]
        exp_local, _, ff = wg_loc.shape
        half = tok // 2
        hbm = pl.BlockSpec(memory_space=pl.ANY)
        vm = pl.BlockSpec(memory_space=pltpu.VMEM)
        dma = pltpu.SemaphoreType.DMA
        out = pltpu.VMEM
        results = pl.pallas_call(
            functools.partial(ring_kernel, n_z),
            out_shape=(out((tok, d_model), BF16), out((tok, d_model), BF16), out((top_k, tok), F32),
                       out(wg_loc.shape, F32), out(wu_loc.shape, F32), out(wd_loc.shape, F32)),
            in_specs=[hbm, hbm, vm, vm, hbm, hbm, hbm],
            out_specs=(vm, vm, vm, vm, vm, vm),
            scratch_shapes=[
                pltpu.VMEM((n, 2, tok, d_model), BF16),
                pltpu.VMEM((n, 2, 2 * top_k, half), F32),
                pltpu.VMEM((SLOTS, 2, tok, d_model), F32),
                pltpu.VMEM((SLOTS, 2, top_k, half), F32),
                pltpu.VMEM((2, tok, d_model), F32),
                pltpu.VMEM((2, top_k, half), F32),
                pltpu.VMEM((tok, d_model), F32),
                pltpu.VMEM((top_k, half), F32),
                pltpu.VMEM(wg_loc.shape, BF16), pltpu.VMEM(wu_loc.shape, BF16), pltpu.VMEM(wd_loc.shape, BF16),
                dma((5,)),
                dma((n, 2)), dma((n, 2)), dma((n, 2)), dma((n, 2)), dma((n, 2)), dma((n, 2)), dma((n, 2)), dma((n, 2)),
                dma((n, 2)), dma((n, 2)), dma((2,)),
                pltpu.SemaphoreType.REGULAR((2,)),
            ],
            compiler_params=pltpu.CompilerParams(collective_id=0, has_side_effects=True, vmem_limit_bytes=48 * 2**20),
        )(x_loc, dy_loc, idx_loc.T, gate_loc.T, wg_loc, wu_loc, wd_loc)
        y, dx, dgate, dwg, dwu, dwd = pl.pallas_call(
            store_kernel,
            out_shape=tuple(jax.ShapeDtypeStruct(r.shape, r.dtype) for r in results),
            in_specs=[vm] * len(results),
            out_specs=(hbm,) * len(results),
            scratch_shapes=[dma((len(results),))],
            compiler_params=pltpu.CompilerParams(vmem_limit_bytes=2**20),
        )(*[pltpu.with_memory_space_constraint(r, pltpu.VMEM) for r in results])
        return y, dx, dgate.T, dwg, dwu, dwd

    return jax.shard_map(device_layer, mesh=mesh, in_specs=(tok_spec, tok_spec, tok_spec, weight_spec, weight_spec, weight_spec, tok_spec), out_specs=(tok_spec, tok_spec, tok_spec, grad_spec, grad_spec, grad_spec), check_vma=False)
```

```python
import functools

import jax
import jax.numpy as jnp
from jax import lax
from jax.experimental import pallas as pl
from jax.experimental.pallas import tpu as pltpu
from jax.sharding import PartitionSpec as P

MESH = pl.DeviceIdType.MESH
F32 = jnp.float32
BF16 = jnp.bfloat16
SLOTS = 4


def mm(p, q, cp, cq):
    return lax.dot_general(p, q, (((cp,), (cq,)), ((), ())), preferred_element_type=F32)


def ring_kernel(n_z, x_ref, dy_ref, idx_ref, gate_ref, wg_ref, wu_ref, wd_ref,
                y_ref, dx_ref, dgate_ref, awg, awu, awd,
                xd, gt, acc, dga, part, dgp, pb, dgb, wg, wu, wd,
                load_sem, xd_send, xd_far, xd_recv, gt_send, gt_far, gt_recv, acc_send, acc_recv, dg_send, dg_recv, pb_recv,
                credit):
    top_k, tok = idx_ref.shape
    half = tok // 2
    exp_local = wg_ref.shape[0]
    n_q = 2 * n_z
    n = 2 * n_q
    z = lax.axis_index('ei')
    eo = lax.axis_index('eo')
    ycoord, core = eo // 2, eo % 2
    q = z + ycoord * (n_q - 1 - 2 * z)
    me = 2 * q + core
    first_expert = (z * 4 + eo) * exp_local

    def device_at(pos):
        pos = lax.rem(pos + 2 * n, n)
        chip, c = pos // 2, pos % 2
        col = chip // n_z
        return {'ei': chip + col * (n_q - 1 - 2 * chip), 'eo': col * 2 + c}

    right, left = device_at(me + 1), device_at(me - 1)
    to = (right, left)
    far = (device_at(me + 2), device_at(me - 2))
    back = (left, right)
    partner = {'ei': z, 'eo': eo + 1 - 2 * core}
    leaves = (core == 1, core == 0)

    loads = [pltpu.make_async_copy(src, dst, load_sem.at[i]) for i, (src, dst) in enumerate(
        ((x_ref, xd.at[0, 0]), (dy_ref, xd.at[0, 1]), (wg_ref, wg), (wu_ref, wu), (wd_ref, wd)))]
    for c in loads:
        c.start()

    barrier = pltpu.get_barrier_semaphore()
    for nb in (left, right) + far:
        pl.semaphore_signal(barrier, inc=1, device_id=nb, device_id_type=MESH)

    for d in range(2):
        gt[0, d, :top_k] = idx_ref[:, d * half:(d + 1) * half].astype(F32)
        gt[0, d, top_k:] = gate_ref[:, d * half:(d + 1) * half]
    pl.semaphore_wait(barrier, 4)
    loads[0].wait()
    loads[1].wait()

    def rows(d):
        return pl.ds(d * half, half)

    def xd_copy(s, d):
        return pltpu.make_async_remote_copy(
            src_ref=xd.at[s, :, rows(d)], dst_ref=xd.at[s + 1, :, rows(d)], send_sem=xd_send.at[s, d],
            recv_sem=xd_recv.at[s, d], device_id=to[d], device_id_type=MESH)

    def gt_copy(s, d):
        return pltpu.make_async_remote_copy(
            src_ref=gt.at[s, d], dst_ref=gt.at[s + 1, d], send_sem=gt_send.at[s, d],
            recv_sem=gt_recv.at[s, d], device_id=to[d], device_id_type=MESH)

    def xd_skip(s, d):
        return pltpu.make_async_remote_copy(
            src_ref=xd.at[s, :, rows(d)], dst_ref=xd.at[s + 2, :, rows(d)], send_sem=xd_far.at[s, d],
            recv_sem=xd_recv.at[s + 1, d], device_id=far[d], device_id_type=MESH)

    def gt_skip(s, d):
        return pltpu.make_async_remote_copy(
            src_ref=gt.at[s, d], dst_ref=gt.at[s + 2, d], send_sem=gt_far.at[s, d],
            recv_sem=gt_recv.at[s + 1, d], device_id=far[d], device_id_type=MESH)

    def acc_copy(s, d):
        return pltpu.make_async_remote_copy(
            src_ref=acc.at[lax.rem(s, SLOTS), d], dst_ref=acc.at[lax.rem(s + 1, SLOTS), d],
            send_sem=acc_send.at[s, d], recv_sem=acc_recv.at[s, d], device_id=to[d], device_id_type=MESH)

    def dg_copy(s, d):
        return pltpu.make_async_remote_copy(
            src_ref=dga.at[lax.rem(s, SLOTS), d], dst_ref=dga.at[lax.rem(s + 1, SLOTS), d],
            send_sem=dg_send.at[s, d], recv_sem=dg_recv.at[s, d], device_id=to[d], device_id_type=MESH)

    def xd_direct(d):
        return pltpu.make_async_remote_copy(
            src_ref=xd.at[0, :, rows(d)], dst_ref=xd.at[n - 1, :, rows(d)], send_sem=xd_send.at[n - 2, d],
            recv_sem=xd_recv.at[n - 2, d], device_id=partner, device_id_type=MESH)

    def gt_direct(d):
        return pltpu.make_async_remote_copy(
            src_ref=gt.at[0, d], dst_ref=gt.at[n - 1, d], send_sem=gt_send.at[n - 2, d],
            recv_sem=gt_recv.at[n - 2, d], device_id=partner, device_id_type=MESH)

    def pb_copy(d):
        return pltpu.make_async_remote_copy(
            src_ref=acc.at[1, d], dst_ref=pb, send_sem=acc_send.at[1, d],
            recv_sem=pb_recv.at[0], device_id=partner, device_id_type=MESH)

    def dgb_copy(d):
        return pltpu.make_async_remote_copy(
            src_ref=dga.at[1, d], dst_ref=dgb, send_sem=dg_send.at[1, d],
            recv_sem=pb_recv.at[1], device_id=partner, device_id_type=MESH)

    def add_part(e, at, val):
        for d in range(2):
            here = pl.ds(at, half)
            part[d, here] = jnp.where(e == 0, 0.0, part[d, here]) + val[d * half:(d + 1) * half]

    def compute(s):
        def columns(first, fill):
            pad = jnp.full((128 - top_k, half), fill, F32)
            return jnp.concatenate(
                [jnp.concatenate([gt[s, d, first:first + top_k], pad], axis=0).T for d in range(2)], axis=0)

        ids, gates = columns(0, -1.0), columns(top_k, 0.0)

        def one(e, carry):
            dgs = carry
            mine = ids == (first_expert + e).astype(F32)
            gcol = jnp.sum(jnp.where(mine, gates, 0.0), axis=1, keepdims=True)
            routed = gcol > 0.0
            x = xd[s, 0]
            a = mm(x, wg[e], 1, 0)
            b = mm(x, wu[e], 1, 0)
            sig = jax.nn.sigmoid(a)
            silu = a * sig
            h = jnp.where(routed, silu * b, 0.0).astype(BF16)
            o = mm(h, wd[e], 1, 0).astype(BF16).astype(F32)
            dyf = xd[s, 1].astype(F32)
            add_part(e, 0, gcol * o)
            dg = jnp.sum(dyf * o, axis=1, keepdims=True)
            dgs = dgs + jnp.where(mine, dg, 0.0)
            g = (gcol * dyf).astype(BF16)
            awd[e] = awd[e] + mm(h, g, 0, 0)
            dh = mm(g, wd[e], 1, 1)
            da = jnp.where(routed, dh * b * sig * (1.0 + a * (1.0 - sig)), 0.0).astype(BF16)
            db = jnp.where(routed, dh * silu, 0.0).astype(BF16)
            awg[e] = awg[e] + mm(x, da, 0, 0)
            awu[e] = awu[e] + mm(x, db, 0, 0)
            dxr = (mm(da, wg[e], 1, 1) + mm(db, wu[e], 1, 1)).astype(BF16).astype(F32)
            add_part(e, half, dxr)
            return dgs

        dgs = lax.fori_loop(0, exp_local, one, jnp.zeros((tok, 128), F32))
        for d in range(2):
            dgp[d] = dgs[d * half:(d + 1) * half].T[:top_k]

    for d in range(2):
        gt_copy(0, d).start()
        xd_copy(0, d).start()
    for d in range(2):
        @pl.when(leaves[d])
        def _(d=d):
            gt_direct(d).start()
            xd_direct(d).start()

    for e in range(exp_local):
        awg[e] = jnp.zeros(awg.shape[1:], F32)
        awu[e] = jnp.zeros(awu.shape[1:], F32)
        awd[e] = jnp.zeros(awd.shape[1:], F32)

    for c in loads[2:]:
        c.wait()

    def step(s, carry):
        slot = lax.rem(s, SLOTS)
        for d in range(2):
            gt_copy(s - 1, d).wait_recv()
            xd_copy(s - 1, d).wait_recv()

            @pl.when(jnp.logical_and(s <= n - 2, jnp.logical_or(s == 1, jnp.logical_not(leaves[d]))))
            def _(d=d):
                gt_copy(s, d).start()
                xd_copy(s, d).start()

            @pl.when(jnp.logical_and(s <= n - 4, jnp.logical_not(leaves[d])))
            def _(d=d):
                gt_skip(s, d).start()
                xd_skip(s, d).start()

        compute(s)

        def pass_on(d):
            fresh = jnp.logical_or(s == 1, jnp.logical_and(s == 2, jnp.logical_not(leaves[d])))

            @pl.when(s >= SLOTS)
            def _():
                pl.semaphore_wait(credit.at[d], 1)

            @pl.when(fresh)
            def _():
                acc[slot, d] = part[d]
                dga[slot, d] = dgp[d]

            @pl.when(jnp.logical_not(fresh))
            def _():
                acc_copy(s - 1, d).wait_recv()
                acc[slot, d] = acc[slot, d] + part[d]
                dg_copy(s - 1, d).wait_recv()
                dga[slot, d] = dga[slot, d] + dgp[d]

            @pl.when(jnp.logical_and(s == 1, leaves[d]))
            def _():
                pb_copy(d).start()
                dgb_copy(d).start()

            @pl.when(jnp.logical_not(jnp.logical_and(s == 1, leaves[d])))
            def _():
                acc_copy(s, d).start()
                dg_copy(s, d).start()

        for d, first in ((0, True), (1, True), (0, False), (1, False)):
            @pl.when(leaves[d] if first else jnp.logical_not(leaves[d]))
            def _(d=d):
                pass_on(d)

        for d in range(2):
            @pl.when(s >= 2)
            def _(d=d):
                acc_copy(s - 1, d).wait_send()
                dg_copy(s - 1, d).wait_send()

            @pl.when(jnp.logical_and(s >= 2, s - 1 + SLOTS <= n))
            def _(d=d):
                pl.semaphore_signal(credit.at[d], inc=1, device_id=back[d], device_id_type=MESH)

        return carry

    lax.fori_loop(1, n, step, 0)

    compute(0)

    def drain(s, carry):
        for d in range(2):
            @pl.when(jnp.logical_or(jnp.logical_or(s <= 1, s == n - 2), jnp.logical_not(leaves[d])))
            def _(d=d):
                gt_copy(s, d).wait_send()
                xd_copy(s, d).wait_send()

            @pl.when(jnp.logical_and(jnp.logical_and(s >= 1, s <= n - 4), jnp.logical_not(leaves[d])))
            def _(d=d):
                gt_skip(s, d).wait_send()
                xd_skip(s, d).wait_send()

        return carry

    lax.fori_loop(0, n - 1, drain, 0)
    last = n % SLOTS
    for d in range(2):
        acc_copy(n - 1, d).wait_send()
        dg_copy(n - 1, d).wait_send()
    pb_copy(0).wait_recv()
    dgb_copy(0).wait_recv()
    for d in range(2):
        dg_copy(n - 1, d).wait_recv()
        dgate_ref[:, d * half:(d + 1) * half] = dga[last, d] + dgp[d] + jnp.where(leaves[d], 0.0, dgb[...])
        acc_copy(n - 1, d).wait_recv()
        for k, out in enumerate((y_ref, dx_ref)):
            here = pl.ds(k * half, half)
            out[rows(d)] = (acc[last, d, here] + part[d, here] + jnp.where(leaves[d], 0.0, pb[here])).astype(BF16)


def store_kernel(*refs):
    count = len(refs) // 2
    sems = refs[-1]
    copies = [pltpu.make_async_copy(refs[i], refs[count + i], sems.at[i]) for i in range(count)]
    for c in copies:
        c.start()
    for c in copies:
        c.wait()


def solution(mesh):
    n_z = mesh.shape['ei']
    n = n_z * mesh.shape['eo']
    tok_spec = P(('dp', 'ei', 'eo'), None)
    weight_spec = P(('ei', 'eo'), None, None)
    grad_spec = P(('dp', 'ei', 'eo'), None, None)

    def device_layer(x_loc, idx_loc, gate_loc, wg_loc, wu_loc, wd_loc, dy_loc):
        tok, top_k = idx_loc.shape
        d_model = x_loc.shape[1]
        exp_local, _, ff = wg_loc.shape
        half = tok // 2
        hbm = pl.BlockSpec(memory_space=pl.ANY)
        vm = pl.BlockSpec(memory_space=pltpu.VMEM)
        dma = pltpu.SemaphoreType.DMA
        out = pltpu.VMEM
        results = pl.pallas_call(
            functools.partial(ring_kernel, n_z),
            out_shape=(out((tok, d_model), BF16), out((tok, d_model), BF16), out((top_k, tok), F32),
                       out(wg_loc.shape, F32), out(wu_loc.shape, F32), out(wd_loc.shape, F32)),
            in_specs=[hbm, hbm, vm, vm, hbm, hbm, hbm],
            out_specs=(vm, vm, vm, vm, vm, vm),
            scratch_shapes=[
                pltpu.VMEM((n, 2, tok, d_model), BF16),
                pltpu.VMEM((n, 2, 2 * top_k, half), F32),
                pltpu.VMEM((SLOTS, 2, tok, d_model), F32),
                pltpu.VMEM((SLOTS, 2, top_k, half), F32),
                pltpu.VMEM((2, tok, d_model), F32),
                pltpu.VMEM((2, top_k, half), F32),
                pltpu.VMEM((tok, d_model), F32),
                pltpu.VMEM((top_k, half), F32),
                pltpu.VMEM(wg_loc.shape, BF16), pltpu.VMEM(wu_loc.shape, BF16), pltpu.VMEM(wd_loc.shape, BF16),
                dma((5,)),
                dma((n, 2)), dma((n, 2)), dma((n, 2)), dma((n, 2)), dma((n, 2)), dma((n, 2)), dma((n, 2)), dma((n, 2)),
                dma((n, 2)), dma((n, 2)), dma((2,)),
                pltpu.SemaphoreType.REGULAR((2,)),
            ],
            compiler_params=pltpu.CompilerParams(collective_id=0, has_side_effects=True, vmem_limit_bytes=48 * 2**20),
        )(x_loc, dy_loc, idx_loc.T, gate_loc.T, wg_loc, wu_loc, wd_loc)
        y, dx, dgate, dwg, dwu, dwd = pl.pallas_call(
            store_kernel,
            out_shape=tuple(jax.ShapeDtypeStruct(r.shape, r.dtype) for r in results),
            in_specs=[vm] * len(results),
            out_specs=(hbm,) * len(results),
            scratch_shapes=[dma((len(results),))],
            compiler_params=pltpu.CompilerParams(vmem_limit_bytes=2**20),
        )(*[pltpu.with_memory_space_constraint(r, pltpu.VMEM) for r in results])
        return y, dx, dgate.T, dwg, dwu, dwd

    return jax.shard_map(device_layer, mesh=mesh, in_specs=(tok_spec, tok_spec, tok_spec, weight_spec, weight_spec, weight_spec, tok_spec), out_specs=(tok_spec, tok_spec, tok_spec, grad_spec, grad_spec, grad_spec), check_vma=False)
```

```python
import functools

import jax
import jax.numpy as jnp
from jax import lax
from jax.experimental import pallas as pl
from jax.experimental.pallas import tpu as pltpu
from jax.sharding import PartitionSpec as P

MESH = pl.DeviceIdType.MESH
F32 = jnp.float32
BF16 = jnp.bfloat16
SLOTS = 4


def mm(p, q, cp, cq):
    return lax.dot_general(p, q, (((cp,), (cq,)), ((), ())), preferred_element_type=F32)


def ring_kernel(n_z, x_ref, dy_ref, idx_ref, gate_ref, wg_ref, wu_ref, wd_ref,
                y_ref, dx_ref, dgate_ref, awg, awu, awd,
                xd, gt, acc, dga, part, dgp, pb, dgb, wg, wu, wd,
                load_sem, xd_send, xd_far, xd_recv, gt_send, gt_far, gt_recv, acc_send, acc_recv, dg_send, dg_recv, pb_recv,
                credit):
    top_k, tok = idx_ref.shape
    half = tok // 2
    exp_local = wg_ref.shape[0]
    n_q = 2 * n_z
    n = 2 * n_q
    z = lax.axis_index('ei')
    eo = lax.axis_index('eo')
    ycoord, core = eo // 2, eo % 2
    q = z + ycoord * (n_q - 1 - 2 * z)
    me = 2 * q + core
    first_expert = (z * 4 + eo) * exp_local

    def device_at(pos):
        pos = lax.rem(pos + 2 * n, n)
        chip, c = pos // 2, pos % 2
        col = chip // n_z
        return {'ei': chip + col * (n_q - 1 - 2 * chip), 'eo': col * 2 + c}

    right, left = device_at(me + 1), device_at(me - 1)
    to = (right, left)
    far = (device_at(me + 2), device_at(me - 2))
    back = (left, right)
    partner = {'ei': z, 'eo': eo + 1 - 2 * core}
    leaves = (core == 1, core == 0)

    loads = [pltpu.make_async_copy(src, dst, load_sem.at[i]) for i, (src, dst) in enumerate(
        ((x_ref, xd.at[0, 0]), (dy_ref, xd.at[0, 1]), (wg_ref, wg), (wu_ref, wu), (wd_ref, wd)))]
    for c in loads:
        c.start()

    barrier = pltpu.get_barrier_semaphore()
    for nb in (left, right) + far:
        pl.semaphore_signal(barrier, inc=1, device_id=nb, device_id_type=MESH)

    for d in range(2):
        gt[0, d, :top_k] = idx_ref[:, d * half:(d + 1) * half].astype(F32)
        gt[0, d, top_k:] = gate_ref[:, d * half:(d + 1) * half]
    pl.semaphore_wait(barrier, 4)
    loads[0].wait()
    loads[1].wait()

    def rows(d):
        return pl.ds(d * half, half)

    def xd_copy(s, d):
        return pltpu.make_async_remote_copy(
            src_ref=xd.at[s, :, rows(d)], dst_ref=xd.at[s + 1, :, rows(d)], send_sem=xd_send.at[s, d],
            recv_sem=xd_recv.at[s, d], device_id=to[d], device_id_type=MESH)

    def gt_copy(s, d):
        return pltpu.make_async_remote_copy(
            src_ref=gt.at[s, d], dst_ref=gt.at[s + 1, d], send_sem=gt_send.at[s, d],
            recv_sem=gt_recv.at[s, d], device_id=to[d], device_id_type=MESH)

    def xd_skip(s, d):
        return pltpu.make_async_remote_copy(
            src_ref=xd.at[s, :, rows(d)], dst_ref=xd.at[s + 2, :, rows(d)], send_sem=xd_far.at[s, d],
            recv_sem=xd_recv.at[s + 1, d], device_id=far[d], device_id_type=MESH)

    def gt_skip(s, d):
        return pltpu.make_async_remote_copy(
            src_ref=gt.at[s, d], dst_ref=gt.at[s + 2, d], send_sem=gt_far.at[s, d],
            recv_sem=gt_recv.at[s + 1, d], device_id=far[d], device_id_type=MESH)

    def acc_copy(s, d):
        return pltpu.make_async_remote_copy(
            src_ref=acc.at[lax.rem(s, SLOTS), d], dst_ref=acc.at[lax.rem(s + 1, SLOTS), d],
            send_sem=acc_send.at[s, d], recv_sem=acc_recv.at[s, d], device_id=to[d], device_id_type=MESH)

    def dg_copy(s, d):
        return pltpu.make_async_remote_copy(
            src_ref=dga.at[lax.rem(s, SLOTS), d], dst_ref=dga.at[lax.rem(s + 1, SLOTS), d],
            send_sem=dg_send.at[s, d], recv_sem=dg_recv.at[s, d], device_id=to[d], device_id_type=MESH)

    def xd_direct(d):
        return pltpu.make_async_remote_copy(
            src_ref=xd.at[0, :, rows(d)], dst_ref=xd.at[n - 1, :, rows(d)], send_sem=xd_send.at[n - 2, d],
            recv_sem=xd_recv.at[n - 2, d], device_id=partner, device_id_type=MESH)

    def gt_direct(d):
        return pltpu.make_async_remote_copy(
            src_ref=gt.at[0, d], dst_ref=gt.at[n - 1, d], send_sem=gt_send.at[n - 2, d],
            recv_sem=gt_recv.at[n - 2, d], device_id=partner, device_id_type=MESH)

    def pb_copy(d):
        return pltpu.make_async_remote_copy(
            src_ref=acc.at[1, d], dst_ref=pb, send_sem=acc_send.at[1, d],
            recv_sem=pb_recv.at[0], device_id=partner, device_id_type=MESH)

    def dgb_copy(d):
        return pltpu.make_async_remote_copy(
            src_ref=dga.at[1, d], dst_ref=dgb, send_sem=dg_send.at[1, d],
            recv_sem=pb_recv.at[1], device_id=partner, device_id_type=MESH)

    def add_part(e, at, val):
        for d in range(2):
            here = pl.ds(at, half)
            part[d, here] = jnp.where(e == 0, 0.0, part[d, here]) + val[d * half:(d + 1) * half]

    def compute(s):
        def columns(first, fill):
            pad = jnp.full((128 - top_k, half), fill, F32)
            return jnp.concatenate(
                [jnp.concatenate([gt[s, d, first:first + top_k], pad], axis=0).T for d in range(2)], axis=0)

        ids, gates = columns(0, -1.0), columns(top_k, 0.0)

        def one(e, carry):
            dgs = carry
            mine = ids == (first_expert + e).astype(F32)
            gcol = jnp.sum(jnp.where(mine, gates, 0.0), axis=1, keepdims=True)
            routed = gcol > 0.0
            x = xd[s, 0]
            a = mm(x, wg[e], 1, 0)
            b = mm(x, wu[e], 1, 0)
            sig = jax.nn.sigmoid(a)
            silu = a * sig
            h = jnp.where(routed, silu * b, 0.0).astype(BF16)
            o = mm(h, wd[e], 1, 0).astype(BF16).astype(F32)
            dyf = xd[s, 1].astype(F32)
            add_part(e, 0, gcol * o)
            dg = jnp.sum(dyf * o, axis=1, keepdims=True)
            dgs = dgs + jnp.where(mine, dg, 0.0)
            g = (gcol * dyf).astype(BF16)
            awd[e] = awd[e] + mm(h, g, 0, 0)
            dh = mm(g, wd[e], 1, 1)
            da = jnp.where(routed, dh * b * sig * (1.0 + a * (1.0 - sig)), 0.0).astype(BF16)
            db = jnp.where(routed, dh * silu, 0.0).astype(BF16)
            awg[e] = awg[e] + mm(x, da, 0, 0)
            awu[e] = awu[e] + mm(x, db, 0, 0)
            dxr = (mm(da, wg[e], 1, 1) + mm(db, wu[e], 1, 1)).astype(BF16).astype(F32)
            add_part(e, half, dxr)
            return dgs

        dgs = lax.fori_loop(0, exp_local, one, jnp.zeros((tok, 128), F32))
        for d in range(2):
            dgp[d] = dgs[d * half:(d + 1) * half].T[:top_k]

    for d in range(2):
        gt_copy(0, d).start()
        xd_copy(0, d).start()
    for d in range(2):
        @pl.when(leaves[d])
        def _(d=d):
            gt_direct(d).start()
            xd_direct(d).start()

    for e in range(exp_local):
        awg[e] = jnp.zeros(awg.shape[1:], F32)
        awu[e] = jnp.zeros(awu.shape[1:], F32)
        awd[e] = jnp.zeros(awd.shape[1:], F32)

    for d in range(2):
        @pl.when(leaves[d])
        def _(d=d):
            gt_copy(0, d).wait_recv()
            xd_copy(0, d).wait_recv()
            gt_copy(1, d).start()
            xd_copy(1, d).start()

    for c in loads[2:]:
        c.wait()

    def step(s, carry):
        slot = lax.rem(s, SLOTS)
        for d in range(2):
            @pl.when(jnp.logical_not(leaves[d]))
            def _(d=d):
                gt_copy(s - 1, d).wait_recv()
                xd_copy(s - 1, d).wait_recv()

                @pl.when(s <= n - 2)
                def _():
                    gt_copy(s, d).start()
                    xd_copy(s, d).start()

                @pl.when(s <= n - 4)
                def _():
                    gt_skip(s, d).start()
                    xd_skip(s, d).start()

        for d in range(2):
            @pl.when(jnp.logical_and(s >= 2, leaves[d]))
            def _(d=d):
                gt_copy(s - 1, d).wait_recv()
                xd_copy(s - 1, d).wait_recv()

        compute(s)

        def pass_on(d):
            fresh = jnp.logical_or(s == 1, jnp.logical_and(s == 2, jnp.logical_not(leaves[d])))

            @pl.when(s >= SLOTS)
            def _():
                pl.semaphore_wait(credit.at[d], 1)

            @pl.when(fresh)
            def _():
                acc[slot, d] = part[d]
                dga[slot, d] = dgp[d]

            @pl.when(jnp.logical_not(fresh))
            def _():
                acc_copy(s - 1, d).wait_recv()
                acc[slot, d] = acc[slot, d] + part[d]
                dg_copy(s - 1, d).wait_recv()
                dga[slot, d] = dga[slot, d] + dgp[d]

            @pl.when(jnp.logical_and(s == 1, leaves[d]))
            def _():
                pb_copy(d).start()
                dgb_copy(d).start()

            @pl.when(jnp.logical_not(jnp.logical_and(s == 1, leaves[d])))
            def _():
                acc_copy(s, d).start()
                dg_copy(s, d).start()

        for d, first in ((0, True), (1, True), (0, False), (1, False)):
            @pl.when(leaves[d] if first else jnp.logical_not(leaves[d]))
            def _(d=d):
                pass_on(d)

        for d in range(2):
            @pl.when(s >= 2)
            def _(d=d):
                acc_copy(s - 1, d).wait_send()
                dg_copy(s - 1, d).wait_send()

            @pl.when(jnp.logical_and(s >= 2, s - 1 + SLOTS <= n))
            def _(d=d):
                pl.semaphore_signal(credit.at[d], inc=1, device_id=back[d], device_id_type=MESH)

        return carry

    lax.fori_loop(1, n, step, 0)

    compute(0)

    def drain(s, carry):
        for d in range(2):
            @pl.when(jnp.logical_or(jnp.logical_or(s <= 1, s == n - 2), jnp.logical_not(leaves[d])))
            def _(d=d):
                gt_copy(s, d).wait_send()
                xd_copy(s, d).wait_send()

            @pl.when(jnp.logical_and(jnp.logical_and(s >= 1, s <= n - 4), jnp.logical_not(leaves[d])))
            def _(d=d):
                gt_skip(s, d).wait_send()
                xd_skip(s, d).wait_send()

        return carry

    lax.fori_loop(0, n - 1, drain, 0)
    last = n % SLOTS
    for d in range(2):
        acc_copy(n - 1, d).wait_send()
        dg_copy(n - 1, d).wait_send()
    pb_copy(0).wait_recv()
    dgb_copy(0).wait_recv()
    for d in range(2):
        dg_copy(n - 1, d).wait_recv()
        dgate_ref[:, d * half:(d + 1) * half] = dga[last, d] + dgp[d] + jnp.where(leaves[d], 0.0, dgb[...])
        acc_copy(n - 1, d).wait_recv()
        for k, out in enumerate((y_ref, dx_ref)):
            here = pl.ds(k * half, half)
            out[rows(d)] = (acc[last, d, here] + part[d, here] + jnp.where(leaves[d], 0.0, pb[here])).astype(BF16)


def store_kernel(*refs):
    count = len(refs) // 2
    sems = refs[-1]
    copies = [pltpu.make_async_copy(refs[i], refs[count + i], sems.at[i]) for i in range(count)]
    for c in copies:
        c.start()
    for c in copies:
        c.wait()


def solution(mesh):
    n_z = mesh.shape['ei']
    n = n_z * mesh.shape['eo']
    tok_spec = P(('dp', 'ei', 'eo'), None)
    weight_spec = P(('ei', 'eo'), None, None)
    grad_spec = P(('dp', 'ei', 'eo'), None, None)

    def device_layer(x_loc, idx_loc, gate_loc, wg_loc, wu_loc, wd_loc, dy_loc):
        tok, top_k = idx_loc.shape
        d_model = x_loc.shape[1]
        exp_local, _, ff = wg_loc.shape
        half = tok // 2
        hbm = pl.BlockSpec(memory_space=pl.ANY)
        vm = pl.BlockSpec(memory_space=pltpu.VMEM)
        dma = pltpu.SemaphoreType.DMA
        out = pltpu.VMEM
        results = pl.pallas_call(
            functools.partial(ring_kernel, n_z),
            out_shape=(out((tok, d_model), BF16), out((tok, d_model), BF16), out((top_k, tok), F32),
                       out(wg_loc.shape, F32), out(wu_loc.shape, F32), out(wd_loc.shape, F32)),
            in_specs=[hbm, hbm, vm, vm, hbm, hbm, hbm],
            out_specs=(vm, vm, vm, vm, vm, vm),
            scratch_shapes=[
                pltpu.VMEM((n, 2, tok, d_model), BF16),
                pltpu.VMEM((n, 2, 2 * top_k, half), F32),
                pltpu.VMEM((SLOTS, 2, tok, d_model), F32),
                pltpu.VMEM((SLOTS, 2, top_k, half), F32),
                pltpu.VMEM((2, tok, d_model), F32),
                pltpu.VMEM((2, top_k, half), F32),
                pltpu.VMEM((tok, d_model), F32),
                pltpu.VMEM((top_k, half), F32),
                pltpu.VMEM(wg_loc.shape, BF16), pltpu.VMEM(wu_loc.shape, BF16), pltpu.VMEM(wd_loc.shape, BF16),
                dma((5,)),
                dma((n, 2)), dma((n, 2)), dma((n, 2)), dma((n, 2)), dma((n, 2)), dma((n, 2)), dma((n, 2)), dma((n, 2)),
                dma((n, 2)), dma((n, 2)), dma((2,)),
                pltpu.SemaphoreType.REGULAR((2,)),
            ],
            compiler_params=pltpu.CompilerParams(collective_id=0, has_side_effects=True, vmem_limit_bytes=48 * 2**20),
        )(x_loc, dy_loc, idx_loc.T, gate_loc.T, wg_loc, wu_loc, wd_loc)
        y, dx, dgate, dwg, dwu, dwd = pl.pallas_call(
            store_kernel,
            out_shape=tuple(jax.ShapeDtypeStruct(r.shape, r.dtype) for r in results),
            in_specs=[vm] * len(results),
            out_specs=(hbm,) * len(results),
            scratch_shapes=[dma((len(results),))],
            compiler_params=pltpu.CompilerParams(vmem_limit_bytes=2**20),
        )(*[pltpu.with_memory_space_constraint(r, pltpu.VMEM) for r in results])
        return y, dx, dgate.T, dwg, dwu, dwd

    return jax.shard_map(device_layer, mesh=mesh, in_specs=(tok_spec, tok_spec, tok_spec, weight_spec, weight_spec, weight_spec, tok_spec), out_specs=(tok_spec, tok_spec, tok_spec, grad_spec, grad_spec, grad_spec), check_vma=False)
```

```python
import functools

import jax
import jax.numpy as jnp
from jax import lax
from jax.experimental import pallas as pl
from jax.experimental.pallas import tpu as pltpu
from jax.sharding import PartitionSpec as P

MESH = pl.DeviceIdType.MESH
F32 = jnp.float32
BF16 = jnp.bfloat16
SLOTS = 4


def mm(p, q, cp, cq):
    return lax.dot_general(p, q, (((cp,), (cq,)), ((), ())), preferred_element_type=F32)


def ring_kernel(n_z, x_ref, dy_ref, idx_ref, gate_ref, wg_ref, wu_ref, wd_ref,
                y_ref, dx_ref, dgate_ref, awg, awu, awd,
                xd, gt, acc, dga, part, dgp, pb, dgb, wg, wu, wd,
                load_sem, xd_send, xd_far, xd_recv, gt_send, gt_far, gt_recv, acc_send, acc_recv, dg_send, dg_recv, pb_recv,
                credit):
    top_k, tok = idx_ref.shape
    half = tok // 2
    exp_local = wg_ref.shape[0]
    n_q = 2 * n_z
    n = 2 * n_q
    z = lax.axis_index('ei')
    eo = lax.axis_index('eo')
    ycoord, core = eo // 2, eo % 2
    q = z + ycoord * (n_q - 1 - 2 * z)
    me = 2 * q + core
    first_expert = (z * 4 + eo) * exp_local

    def device_at(pos):
        pos = lax.rem(pos + 2 * n, n)
        chip, c = pos // 2, pos % 2
        col = chip // n_z
        return {'ei': chip + col * (n_q - 1 - 2 * chip), 'eo': col * 2 + c}

    right, left = device_at(me + 1), device_at(me - 1)
    to = (right, left)
    far = (device_at(me + 2), device_at(me - 2))
    back = (left, right)
    partner = {'ei': z, 'eo': eo + 1 - 2 * core}
    leaves = (core == 1, core == 0)

    loads = [pltpu.make_async_copy(src, dst, load_sem.at[i]) for i, (src, dst) in enumerate(
        ((x_ref, xd.at[0, 0]), (dy_ref, xd.at[0, 1]), (wg_ref, wg), (wu_ref, wu), (wd_ref, wd)))]
    for c in loads:
        c.start()

    barrier = pltpu.get_barrier_semaphore()
    for nb in (left, right) + far:
        pl.semaphore_signal(barrier, inc=1, device_id=nb, device_id_type=MESH)

    for d in range(2):
        gt[0, d, :top_k] = idx_ref[:, d * half:(d + 1) * half].astype(F32)
        gt[0, d, top_k:] = gate_ref[:, d * half:(d + 1) * half]
    pl.semaphore_wait(barrier, 4)
    loads[0].wait()
    loads[1].wait()

    def rows(d):
        return pl.ds(d * half, half)

    def xd_copy(s, d):
        return pltpu.make_async_remote_copy(
            src_ref=xd.at[s, :, rows(d)], dst_ref=xd.at[s + 1, :, rows(d)], send_sem=xd_send.at[s, d],
            recv_sem=xd_recv.at[s, d], device_id=to[d], device_id_type=MESH)

    def gt_copy(s, d):
        return pltpu.make_async_remote_copy(
            src_ref=gt.at[s, d], dst_ref=gt.at[s + 1, d], send_sem=gt_send.at[s, d],
            recv_sem=gt_recv.at[s, d], device_id=to[d], device_id_type=MESH)

    def xd_skip(s, d):
        return pltpu.make_async_remote_copy(
            src_ref=xd.at[s, :, rows(d)], dst_ref=xd.at[s + 2, :, rows(d)], send_sem=xd_far.at[s, d],
            recv_sem=xd_recv.at[s + 1, d], device_id=far[d], device_id_type=MESH)

    def gt_skip(s, d):
        return pltpu.make_async_remote_copy(
            src_ref=gt.at[s, d], dst_ref=gt.at[s + 2, d], send_sem=gt_far.at[s, d],
            recv_sem=gt_recv.at[s + 1, d], device_id=far[d], device_id_type=MESH)

    def acc_copy(s, d):
        return pltpu.make_async_remote_copy(
            src_ref=acc.at[lax.rem(s, SLOTS), d], dst_ref=acc.at[lax.rem(s + 1, SLOTS), d],
            send_sem=acc_send.at[s, d], recv_sem=acc_recv.at[s, d], device_id=to[d], device_id_type=MESH)

    def dg_copy(s, d):
        return pltpu.make_async_remote_copy(
            src_ref=dga.at[lax.rem(s, SLOTS), d], dst_ref=dga.at[lax.rem(s + 1, SLOTS), d],
            send_sem=dg_send.at[s, d], recv_sem=dg_recv.at[s, d], device_id=to[d], device_id_type=MESH)

    def xd_direct(d):
        return pltpu.make_async_remote_copy(
            src_ref=xd.at[0, :, rows(d)], dst_ref=xd.at[n - 1, :, rows(d)], send_sem=xd_send.at[n - 2, d],
            recv_sem=xd_recv.at[n - 2, d], device_id=partner, device_id_type=MESH)

    def gt_direct(d):
        return pltpu.make_async_remote_copy(
            src_ref=gt.at[0, d], dst_ref=gt.at[n - 1, d], send_sem=gt_send.at[n - 2, d],
            recv_sem=gt_recv.at[n - 2, d], device_id=partner, device_id_type=MESH)

    def pb_copy(d):
        return pltpu.make_async_remote_copy(
            src_ref=acc.at[1, d], dst_ref=pb, send_sem=acc_send.at[1, d],
            recv_sem=pb_recv.at[0], device_id=partner, device_id_type=MESH)

    def dgb_copy(d):
        return pltpu.make_async_remote_copy(
            src_ref=dga.at[1, d], dst_ref=dgb, send_sem=dg_send.at[1, d],
            recv_sem=pb_recv.at[1], device_id=partner, device_id_type=MESH)

    def add_part(e, at, val):
        for d in range(2):
            here = pl.ds(at, half)
            part[d, here] = jnp.where(e == 0, 0.0, part[d, here]) + val[d * half:(d + 1) * half]

    def compute(s):
        def columns(first, fill):
            pad = jnp.full((128 - top_k, half), fill, F32)
            return jnp.concatenate(
                [jnp.concatenate([gt[s, d, first:first + top_k], pad], axis=0).T for d in range(2)], axis=0)

        ids, gates = columns(0, -1.0), columns(top_k, 0.0)

        def one(e, carry):
            dgs = carry
            mine = ids == (first_expert + e).astype(F32)
            gcol = jnp.sum(jnp.where(mine, gates, 0.0), axis=1, keepdims=True)
            routed = gcol > 0.0
            x = xd[s, 0]
            a = mm(x, wg[e], 1, 0)
            b = mm(x, wu[e], 1, 0)
            sig = jax.nn.sigmoid(a)
            silu = a * sig
            h = jnp.where(routed, silu * b, 0.0).astype(BF16)
            o = mm(h, wd[e], 1, 0).astype(BF16).astype(F32)
            dyf = xd[s, 1].astype(F32)
            add_part(e, 0, gcol * o)
            dg = jnp.sum(dyf * o, axis=1, keepdims=True)
            dgs = dgs + jnp.where(mine, dg, 0.0)
            g = (gcol * dyf).astype(BF16)
            awd[e] = awd[e] + mm(h, g, 0, 0)
            dh = mm(g, wd[e], 1, 1)
            da = jnp.where(routed, dh * b * sig * (1.0 + a * (1.0 - sig)), 0.0).astype(BF16)
            db = jnp.where(routed, dh * silu, 0.0).astype(BF16)
            awg[e] = awg[e] + mm(x, da, 0, 0)
            awu[e] = awu[e] + mm(x, db, 0, 0)
            dxr = (mm(da, wg[e], 1, 1) + mm(db, wu[e], 1, 1)).astype(BF16).astype(F32)
            add_part(e, half, dxr)
            return dgs

        dgs = lax.fori_loop(0, exp_local, one, jnp.zeros((tok, 128), F32))
        for d in range(2):
            dgp[d] = dgs[d * half:(d + 1) * half].T[:top_k]

    for d in range(2):
        gt_copy(0, d).start()
        xd_copy(0, d).start()
    for d in range(2):
        @pl.when(leaves[d])
        def _(d=d):
            gt_direct(d).start()
            xd_direct(d).start()

    for e in range(exp_local):
        awg[e] = jnp.zeros(awg.shape[1:], F32)
        awu[e] = jnp.zeros(awu.shape[1:], F32)
        awd[e] = jnp.zeros(awd.shape[1:], F32)

    for d in range(2):
        @pl.when(leaves[d])
        def _(d=d):
            gt_copy(0, d).wait_recv()
            xd_copy(0, d).wait_recv()
            gt_copy(1, d).start()
            xd_copy(1, d).start()

    for c in loads[2:]:
        c.wait()

    def step(s, carry):
        slot = lax.rem(s, SLOTS)
        for d in range(2):
            @pl.when(jnp.logical_not(leaves[d]))
            def _(d=d):
                gt_copy(s - 1, d).wait_recv()
                xd_copy(s - 1, d).wait_recv()

                @pl.when(s <= n - 2)
                def _():
                    gt_copy(s, d).start()
                    xd_copy(s, d).start()

                @pl.when(s <= n - 4)
                def _():
                    gt_skip(s, d).start()
                    xd_skip(s, d).start()

        for d in range(2):
            @pl.when(jnp.logical_and(s >= 2, leaves[d]))
            def _(d=d):
                gt_copy(s - 1, d).wait_recv()
                xd_copy(s - 1, d).wait_recv()

        compute(s)

        def pass_on(d):
            fresh = jnp.logical_or(s == 1, jnp.logical_and(s == 2, jnp.logical_not(leaves[d])))

            @pl.when(s >= SLOTS)
            def _():
                pl.semaphore_wait(credit.at[d], 1)

            @pl.when(fresh)
            def _():
                acc[slot, d] = part[d]
                dga[slot, d] = dgp[d]

            @pl.when(jnp.logical_not(fresh))
            def _():
                acc_copy(s - 1, d).wait_recv()
                acc[slot, d] = acc[slot, d] + part[d]
                dg_copy(s - 1, d).wait_recv()
                dga[slot, d] = dga[slot, d] + dgp[d]

            @pl.when(jnp.logical_and(s == 1, leaves[d]))
            def _():
                pb_copy(d).start()
                dgb_copy(d).start()

            @pl.when(jnp.logical_not(jnp.logical_and(s == 1, leaves[d])))
            def _():
                acc_copy(s, d).start()
                dg_copy(s, d).start()

        for d, first in ((0, True), (1, True), (0, False), (1, False)):
            @pl.when(leaves[d] if first else jnp.logical_not(leaves[d]))
            def _(d=d):
                pass_on(d)

        for d in range(2):
            @pl.when(s >= 2)
            def _(d=d):
                acc_copy(s - 1, d).wait_send()
                dg_copy(s - 1, d).wait_send()

            @pl.when(jnp.logical_and(s >= 2, s - 1 + SLOTS <= n))
            def _(d=d):
                pl.semaphore_signal(credit.at[d], inc=1, device_id=back[d], device_id_type=MESH)

        return carry

    lax.fori_loop(1, n, step, 0)

    compute(0)

    def drain(s, carry):
        for d in range(2):
            @pl.when(jnp.logical_or(jnp.logical_or(s <= 1, s == n - 2), jnp.logical_not(leaves[d])))
            def _(d=d):
                gt_copy(s, d).wait_send()
                xd_copy(s, d).wait_send()

            @pl.when(jnp.logical_and(jnp.logical_and(s >= 1, s <= n - 4), jnp.logical_not(leaves[d])))
            def _(d=d):
                gt_skip(s, d).wait_send()
                xd_skip(s, d).wait_send()

        return carry

    lax.fori_loop(0, n - 1, drain, 0)
    last = n % SLOTS
    pb_copy(0).wait_recv()
    dgb_copy(0).wait_recv()

    def finish(d, extra, dg_extra):
        dg_copy(n - 1, d).wait_recv()
        dgate_ref[:, d * half:(d + 1) * half] = dga[last, d] + dgp[d] + dg_extra
        acc_copy(n - 1, d).wait_recv()
        for k, out in enumerate((y_ref, dx_ref)):
            here = pl.ds(k * half, half)
            out[rows(d)] = (acc[last, d, here] + part[d, here] + extra(here)).astype(BF16)

    for d in range(2):
        @pl.when(leaves[d])
        def _(d=d):
            finish(d, lambda here: 0.0, 0.0)

    for d in range(2):
        @pl.when(jnp.logical_not(leaves[d]))
        def _(d=d):
            finish(d, lambda here: pb[here], dgb[...])

    for d in range(2):
        acc_copy(n - 1, d).wait_send()
        dg_copy(n - 1, d).wait_send()


def store_kernel(*refs):
    count = len(refs) // 2
    sems = refs[-1]
    copies = [pltpu.make_async_copy(refs[i], refs[count + i], sems.at[i]) for i in range(count)]
    for c in copies:
        c.start()
    for c in copies:
        c.wait()


def solution(mesh):
    n_z = mesh.shape['ei']
    n = n_z * mesh.shape['eo']
    tok_spec = P(('dp', 'ei', 'eo'), None)
    weight_spec = P(('ei', 'eo'), None, None)
    grad_spec = P(('dp', 'ei', 'eo'), None, None)

    def device_layer(x_loc, idx_loc, gate_loc, wg_loc, wu_loc, wd_loc, dy_loc):
        tok, top_k = idx_loc.shape
        d_model = x_loc.shape[1]
        exp_local, _, ff = wg_loc.shape
        half = tok // 2
        hbm = pl.BlockSpec(memory_space=pl.ANY)
        vm = pl.BlockSpec(memory_space=pltpu.VMEM)
        dma = pltpu.SemaphoreType.DMA
        out = pltpu.VMEM
        results = pl.pallas_call(
            functools.partial(ring_kernel, n_z),
            out_shape=(out((tok, d_model), BF16), out((tok, d_model), BF16), out((top_k, tok), F32),
                       out(wg_loc.shape, F32), out(wu_loc.shape, F32), out(wd_loc.shape, F32)),
            in_specs=[hbm, hbm, vm, vm, hbm, hbm, hbm],
            out_specs=(vm, vm, vm, vm, vm, vm),
            scratch_shapes=[
                pltpu.VMEM((n, 2, tok, d_model), BF16),
                pltpu.VMEM((n, 2, 2 * top_k, half), F32),
                pltpu.VMEM((SLOTS, 2, tok, d_model), F32),
                pltpu.VMEM((SLOTS, 2, top_k, half), F32),
                pltpu.VMEM((2, tok, d_model), F32),
                pltpu.VMEM((2, top_k, half), F32),
                pltpu.VMEM((tok, d_model), F32),
                pltpu.VMEM((top_k, half), F32),
                pltpu.VMEM(wg_loc.shape, BF16), pltpu.VMEM(wu_loc.shape, BF16), pltpu.VMEM(wd_loc.shape, BF16),
                dma((5,)),
                dma((n, 2)), dma((n, 2)), dma((n, 2)), dma((n, 2)), dma((n, 2)), dma((n, 2)), dma((n, 2)), dma((n, 2)),
                dma((n, 2)), dma((n, 2)), dma((2,)),
                pltpu.SemaphoreType.REGULAR((2,)),
            ],
            compiler_params=pltpu.CompilerParams(collective_id=0, has_side_effects=True, vmem_limit_bytes=48 * 2**20),
        )(x_loc, dy_loc, idx_loc.T, gate_loc.T, wg_loc, wu_loc, wd_loc)
        y, dx, dgate, dwg, dwu, dwd = pl.pallas_call(
            store_kernel,
            out_shape=tuple(jax.ShapeDtypeStruct(r.shape, r.dtype) for r in results),
            in_specs=[vm] * len(results),
            out_specs=(hbm,) * len(results),
            scratch_shapes=[dma((len(results),))],
            compiler_params=pltpu.CompilerParams(vmem_limit_bytes=2**20),
        )(*[pltpu.with_memory_space_constraint(r, pltpu.VMEM) for r in results])
        return y, dx, dgate.T, dwg, dwu, dwd

    return jax.shard_map(device_layer, mesh=mesh, in_specs=(tok_spec, tok_spec, tok_spec, weight_spec, weight_spec, weight_spec, tok_spec), out_specs=(tok_spec, tok_spec, tok_spec, grad_spec, grad_spec, grad_spec), check_vma=False)
```

```python
import functools

import jax
import jax.numpy as jnp
from jax import lax
from jax.experimental import pallas as pl
from jax.experimental.pallas import tpu as pltpu
from jax.sharding import PartitionSpec as P

MESH = pl.DeviceIdType.MESH
F32 = jnp.float32
BF16 = jnp.bfloat16
SLOTS = 4


def mm(p, q, cp, cq):
    return lax.dot_general(p, q, (((cp,), (cq,)), ((), ())), preferred_element_type=F32)


def ring_kernel(n_z, x_ref, dy_ref, idx_ref, gate_ref, wg_ref, wu_ref, wd_ref,
                y_ref, dx_ref, dgate_ref, awg, awu, awd,
                xd, gt, acc, dga, part, dgp, pb, dgb, wg, wu, wd,
                load_sem, xd_send, xd_far, xd_recv, gt_send, gt_far, gt_recv, acc_send, acc_recv, dg_send, dg_recv, pb_recv,
                credit):
    top_k, tok = idx_ref.shape
    half = tok // 2
    exp_local = wg_ref.shape[0]
    n_q = 2 * n_z
    n = 2 * n_q
    z = lax.axis_index('ei')
    eo = lax.axis_index('eo')
    ycoord, core = eo // 2, eo % 2
    q = z + ycoord * (n_q - 1 - 2 * z)
    me = 2 * q + core
    first_expert = (z * 4 + eo) * exp_local

    def device_at(pos):
        pos = lax.rem(pos + 2 * n, n)
        chip, c = pos // 2, pos % 2
        col = chip // n_z
        return {'ei': chip + col * (n_q - 1 - 2 * chip), 'eo': col * 2 + c}

    right, left = device_at(me + 1), device_at(me - 1)
    to = (right, left)
    far = (device_at(me + 2), device_at(me - 2))
    back = (left, right)
    partner = {'ei': z, 'eo': eo + 1 - 2 * core}
    leaves = (core == 1, core == 0)

    loads = [pltpu.make_async_copy(src, dst, load_sem.at[i]) for i, (src, dst) in enumerate(
        ((x_ref, xd.at[0, 0]), (dy_ref, xd.at[0, 1]), (wg_ref, wg), (wu_ref, wu), (wd_ref, wd)))]
    for c in loads:
        c.start()

    barrier = pltpu.get_barrier_semaphore()
    for nb in (left, right) + far:
        pl.semaphore_signal(barrier, inc=1, device_id=nb, device_id_type=MESH)

    for d in range(2):
        gt[0, d, :top_k] = idx_ref[:, d * half:(d + 1) * half].astype(F32)
        gt[0, d, top_k:] = gate_ref[:, d * half:(d + 1) * half]
    pl.semaphore_wait(barrier, 4)
    loads[0].wait()
    loads[1].wait()

    def rows(d):
        return pl.ds(d * half, half)

    def xd_copy(s, d):
        return pltpu.make_async_remote_copy(
            src_ref=xd.at[s, :, rows(d)], dst_ref=xd.at[s + 1, :, rows(d)], send_sem=xd_send.at[s, d],
            recv_sem=xd_recv.at[s, d], device_id=to[d], device_id_type=MESH)

    def gt_copy(s, d):
        return pltpu.make_async_remote_copy(
            src_ref=gt.at[s, d], dst_ref=gt.at[s + 1, d], send_sem=gt_send.at[s, d],
            recv_sem=gt_recv.at[s, d], device_id=to[d], device_id_type=MESH)

    def xd_skip(s, d):
        return pltpu.make_async_remote_copy(
            src_ref=xd.at[s, :, rows(d)], dst_ref=xd.at[s + 2, :, rows(d)], send_sem=xd_far.at[s, d],
            recv_sem=xd_recv.at[s + 1, d], device_id=far[d], device_id_type=MESH)

    def gt_skip(s, d):
        return pltpu.make_async_remote_copy(
            src_ref=gt.at[s, d], dst_ref=gt.at[s + 2, d], send_sem=gt_far.at[s, d],
            recv_sem=gt_recv.at[s + 1, d], device_id=far[d], device_id_type=MESH)

    def acc_copy(s, d):
        return pltpu.make_async_remote_copy(
            src_ref=acc.at[lax.rem(s, SLOTS), d], dst_ref=acc.at[lax.rem(s + 1, SLOTS), d],
            send_sem=acc_send.at[s, d], recv_sem=acc_recv.at[s, d], device_id=to[d], device_id_type=MESH)

    def dg_copy(s, d):
        return pltpu.make_async_remote_copy(
            src_ref=dga.at[lax.rem(s, SLOTS), d], dst_ref=dga.at[lax.rem(s + 1, SLOTS), d],
            send_sem=dg_send.at[s, d], recv_sem=dg_recv.at[s, d], device_id=to[d], device_id_type=MESH)

    def xd_direct(d):
        return pltpu.make_async_remote_copy(
            src_ref=xd.at[0, :, rows(d)], dst_ref=xd.at[n - 1, :, rows(d)], send_sem=xd_send.at[n - 2, d],
            recv_sem=xd_recv.at[n - 2, d], device_id=partner, device_id_type=MESH)

    def gt_direct(d):
        return pltpu.make_async_remote_copy(
            src_ref=gt.at[0, d], dst_ref=gt.at[n - 1, d], send_sem=gt_send.at[n - 2, d],
            recv_sem=gt_recv.at[n - 2, d], device_id=partner, device_id_type=MESH)

    def pb_copy(d):
        return pltpu.make_async_remote_copy(
            src_ref=acc.at[1, d], dst_ref=pb, send_sem=acc_send.at[1, d],
            recv_sem=pb_recv.at[0], device_id=partner, device_id_type=MESH)

    def dgb_copy(d):
        return pltpu.make_async_remote_copy(
            src_ref=dga.at[1, d], dst_ref=dgb, send_sem=dg_send.at[1, d],
            recv_sem=pb_recv.at[1], device_id=partner, device_id_type=MESH)

    def add_part(e, at, val):
        for d in range(2):
            here = pl.ds(at, half)
            part[d, here] = jnp.where(e == 0, 0.0, part[d, here]) + val[d * half:(d + 1) * half]

    def compute(s):
        def columns(first, fill):
            pad = jnp.full((128 - top_k, half), fill, F32)
            return jnp.concatenate(
                [jnp.concatenate([gt[s, d, first:first + top_k], pad], axis=0).T for d in range(2)], axis=0)

        ids, gates = columns(0, -1.0), columns(top_k, 0.0)

        def one(e, carry):
            dgs = carry
            mine = ids == (first_expert + e).astype(F32)
            gcol = jnp.sum(jnp.where(mine, gates, 0.0), axis=1, keepdims=True)
            routed = gcol > 0.0
            x = xd[s, 0]
            a = mm(x, wg[e], 1, 0)
            b = mm(x, wu[e], 1, 0)
            sig = jax.nn.sigmoid(a)
            silu = a * sig
            h = jnp.where(routed, silu * b, 0.0).astype(BF16)
            o = mm(h, wd[e], 1, 0).astype(BF16).astype(F32)
            dyf = xd[s, 1].astype(F32)
            add_part(e, 0, gcol * o)
            dg = jnp.sum(dyf * o, axis=1, keepdims=True)
            dgs = dgs + jnp.where(mine, dg, 0.0)
            g = (gcol * dyf).astype(BF16)
            awd[e] = awd[e] + mm(h, g, 0, 0)
            dh = mm(g, wd[e], 1, 1)
            da = jnp.where(routed, dh * b * sig * (1.0 + a * (1.0 - sig)), 0.0).astype(BF16)
            db = jnp.where(routed, dh * silu, 0.0).astype(BF16)
            awg[e] = awg[e] + mm(x, da, 0, 0)
            awu[e] = awu[e] + mm(x, db, 0, 0)
            dxr = (mm(da, wg[e], 1, 1) + mm(db, wu[e], 1, 1)).astype(BF16).astype(F32)
            add_part(e, half, dxr)
            return dgs

        dgs = lax.fori_loop(0, exp_local, one, jnp.zeros((tok, 128), F32))
        for d in range(2):
            dgp[d] = dgs[d * half:(d + 1) * half].T[:top_k]

    for d in range(2):
        gt_copy(0, d).start()
        xd_copy(0, d).start()
    for d in range(2):
        @pl.when(leaves[d])
        def _(d=d):
            gt_direct(d).start()
            xd_direct(d).start()

    for e in range(exp_local):
        awg[e] = jnp.zeros(awg.shape[1:], F32)
        awu[e] = jnp.zeros(awu.shape[1:], F32)
        awd[e] = jnp.zeros(awd.shape[1:], F32)

    for d in range(2):
        @pl.when(leaves[d])
        def _(d=d):
            gt_copy(0, d).wait_recv()
            xd_copy(0, d).wait_recv()
            gt_copy(1, d).start()
            xd_copy(1, d).start()

    for c in loads[2:]:
        c.wait()

    def step(s, carry):
        slot = lax.rem(s, SLOTS)
        for d in range(2):
            @pl.when(jnp.logical_not(leaves[d]))
            def _(d=d):
                gt_copy(s - 1, d).wait_recv()
                xd_copy(s - 1, d).wait_recv()

                @pl.when(s <= n - 2)
                def _():
                    gt_copy(s, d).start()
                    xd_copy(s, d).start()

                @pl.when(s <= n - 4)
                def _():
                    gt_skip(s, d).start()
                    xd_skip(s, d).start()

        for d in range(2):
            @pl.when(jnp.logical_and(s >= 2, leaves[d]))
            def _(d=d):
                gt_copy(s - 1, d).wait_recv()
                xd_copy(s - 1, d).wait_recv()

        compute(s)

        def pass_on(d):
            fresh = jnp.logical_or(s == 1, jnp.logical_and(s == 2, jnp.logical_not(leaves[d])))

            @pl.when(s >= SLOTS)
            def _():
                pl.semaphore_wait(credit.at[d], 1)

            @pl.when(fresh)
            def _():
                acc[slot, d] = part[d]
                dga[slot, d] = dgp[d]

            @pl.when(jnp.logical_not(fresh))
            def _():
                acc_copy(s - 1, d).wait_recv()
                acc[slot, d] = acc[slot, d] + part[d]
                dg_copy(s - 1, d).wait_recv()
                dga[slot, d] = dga[slot, d] + dgp[d]

            @pl.when(jnp.logical_and(s == 1, leaves[d]))
            def _():
                pb_copy(d).start()
                dgb_copy(d).start()

            @pl.when(jnp.logical_not(jnp.logical_and(s == 1, leaves[d])))
            def _():
                acc_copy(s, d).start()
                dg_copy(s, d).start()

        for d, first in ((0, True), (1, True), (0, False), (1, False)):
            @pl.when(leaves[d] if first else jnp.logical_not(leaves[d]))
            def _(d=d):
                pass_on(d)

        for d in range(2):
            @pl.when(s >= 2)
            def _(d=d):
                acc_copy(s - 1, d).wait_send()
                dg_copy(s - 1, d).wait_send()

            @pl.when(jnp.logical_and(s >= 2, s - 1 + SLOTS <= n))
            def _(d=d):
                pl.semaphore_signal(credit.at[d], inc=1, device_id=back[d], device_id_type=MESH)

        return carry

    lax.fori_loop(1, n, step, 0)

    compute(0)

    def drain(s, carry):
        for d in range(2):
            @pl.when(jnp.logical_or(jnp.logical_or(s <= 1, s == n - 2), jnp.logical_not(leaves[d])))
            def _(d=d):
                gt_copy(s, d).wait_send()
                xd_copy(s, d).wait_send()

            @pl.when(jnp.logical_and(jnp.logical_and(s >= 1, s <= n - 4), jnp.logical_not(leaves[d])))
            def _(d=d):
                gt_skip(s, d).wait_send()
                xd_skip(s, d).wait_send()

        return carry

    lax.fori_loop(0, n - 1, drain, 0)
    last = n % SLOTS
    pb_copy(0).wait_recv()
    dgb_copy(0).wait_recv()

    def finish(d, extra, dg_extra):
        dg_copy(n - 1, d).wait_recv()
        dgate_ref[:, d * half:(d + 1) * half] = dga[last, d] + dgp[d] + dg_extra
        acc_copy(n - 1, d).wait_recv()
        for k, out in enumerate((y_ref, dx_ref)):
            here = pl.ds(k * half, half)
            out[rows(d)] = (acc[last, d, here] + part[d, here] + extra(here)).astype(BF16)

    for d in range(2):
        @pl.when(leaves[d])
        def _(d=d):
            finish(d, lambda here: 0.0, 0.0)

    for d in range(2):
        @pl.when(jnp.logical_not(leaves[d]))
        def _(d=d):
            finish(d, lambda here: pb[here], dgb[...])

    for d in range(2):
        acc_copy(n - 1, d).wait_send()
        dg_copy(n - 1, d).wait_send()


def store_kernel(*refs):
    count = len(refs) // 2
    sems = refs[-1]
    pairs = []
    for src, dst in zip(refs[:count], refs[count:2 * count]):
        if len(src.shape) == 3:
            pairs += [(src.at[e], dst.at[e]) for e in range(src.shape[0])]
        else:
            pairs.append((src, dst))
    copies = [pltpu.make_async_copy(src, dst, sems.at[i]) for i, (src, dst) in enumerate(pairs)]
    for c in copies:
        c.start()
    for c in copies:
        c.wait()


def solution(mesh):
    n_z = mesh.shape['ei']
    n = n_z * mesh.shape['eo']
    tok_spec = P(('dp', 'ei', 'eo'), None)
    weight_spec = P(('ei', 'eo'), None, None)
    grad_spec = P(('dp', 'ei', 'eo'), None, None)

    def device_layer(x_loc, idx_loc, gate_loc, wg_loc, wu_loc, wd_loc, dy_loc):
        tok, top_k = idx_loc.shape
        d_model = x_loc.shape[1]
        exp_local, _, ff = wg_loc.shape
        half = tok // 2
        hbm = pl.BlockSpec(memory_space=pl.ANY)
        vm = pl.BlockSpec(memory_space=pltpu.VMEM)
        dma = pltpu.SemaphoreType.DMA
        out = pltpu.VMEM
        results = pl.pallas_call(
            functools.partial(ring_kernel, n_z),
            out_shape=(out((tok, d_model), BF16), out((tok, d_model), BF16), out((top_k, tok), F32),
                       out(wg_loc.shape, F32), out(wu_loc.shape, F32), out(wd_loc.shape, F32)),
            in_specs=[hbm, hbm, vm, vm, hbm, hbm, hbm],
            out_specs=(vm, vm, vm, vm, vm, vm),
            scratch_shapes=[
                pltpu.VMEM((n, 2, tok, d_model), BF16),
                pltpu.VMEM((n, 2, 2 * top_k, half), F32),
                pltpu.VMEM((SLOTS, 2, tok, d_model), F32),
                pltpu.VMEM((SLOTS, 2, top_k, half), F32),
                pltpu.VMEM((2, tok, d_model), F32),
                pltpu.VMEM((2, top_k, half), F32),
                pltpu.VMEM((tok, d_model), F32),
                pltpu.VMEM((top_k, half), F32),
                pltpu.VMEM(wg_loc.shape, BF16), pltpu.VMEM(wu_loc.shape, BF16), pltpu.VMEM(wd_loc.shape, BF16),
                dma((5,)),
                dma((n, 2)), dma((n, 2)), dma((n, 2)), dma((n, 2)), dma((n, 2)), dma((n, 2)), dma((n, 2)), dma((n, 2)),
                dma((n, 2)), dma((n, 2)), dma((2,)),
                pltpu.SemaphoreType.REGULAR((2,)),
            ],
            compiler_params=pltpu.CompilerParams(collective_id=0, has_side_effects=True, vmem_limit_bytes=48 * 2**20),
        )(x_loc, dy_loc, idx_loc.T, gate_loc.T, wg_loc, wu_loc, wd_loc)
        y, dx, dgate, dwg, dwu, dwd = pl.pallas_call(
            store_kernel,
            out_shape=tuple(jax.ShapeDtypeStruct(r.shape, r.dtype) for r in results),
            in_specs=[vm] * len(results),
            out_specs=(hbm,) * len(results),
            scratch_shapes=[dma((3 + 3 * exp_local,))],
            compiler_params=pltpu.CompilerParams(vmem_limit_bytes=2**20),
        )(*[pltpu.with_memory_space_constraint(r, pltpu.VMEM) for r in results])
        return y, dx, dgate.T, dwg, dwu, dwd

    return jax.shard_map(device_layer, mesh=mesh, in_specs=(tok_spec, tok_spec, tok_spec, weight_spec, weight_spec, weight_spec, tok_spec), out_specs=(tok_spec, tok_spec, tok_spec, grad_spec, grad_spec, grad_spec), check_vma=False)
```
